32 devices in a mesh: pp: 4 (over z), ep: 8 (over y, x, core).
Axes of the slice: x: 2, y: 2, z: 4, core: 2. Of those that a mesh axis runs over, the one named last changes fastest.
Arguments:
- x_fwd: bfloat16 [4, 4096, 512], P('pp', 'ep')
- x_bwd: bfloat16 [4, 4096, 512], P('pp', 'ep')
- grad_in: bfloat16 [4, 4096, 512], P('pp', 'ep')
- dense_in: bfloat16 [4, 2, 512, 1024], P('pp')
- dense_out: bfloat16 [4, 2, 1024, 512], P('pp')
- exp_gate: bfloat16 [4, 2, 64, 512, 256], P('pp', None, 'ep')
- exp_up: bfloat16 [4, 2, 64, 512, 256], P('pp', None, 'ep')
- exp_down: bfloat16 [4, 2, 64, 256, 512], P('pp', None, 'ep')
- route_fwd: int32 [4, 2, 4096, 8], P('pp', None, 'ep')
- gate_fwd: bfloat16 [4, 2, 4096, 8], P('pp', None, 'ep')
- route_bwd: int32 [4, 2, 4096, 8], P('pp', None, 'ep')
- gate_bwd: bfloat16 [4, 2, 4096, 8], P('pp', None, 'ep')
Outputs:
- output 1: bfloat16 [4, 4096, 512], P('pp', 'ep')
- output 2: bfloat16 [4, 4096, 512], P('pp', 'ep')
- output 3: float32 [4, 2, 64, 512, 256], P('pp', None, 'ep')
- output 4: float32 [4, 2, 64, 512, 256], P('pp', None, 'ep')
- output 5: float32 [4, 2, 64, 256, 512], P('pp', None, 'ep')
All inputs are finite; a program needn't handle non-finite values.
Results may differ from the reference program's by a relative error of at most 0.0180287.
Values are sent between devices in bfloat16 or wider.
A program may use at most 1 GiB of HBM per device.

```python
import jax
import jax.numpy as jnp
from jax import lax

STAGES = 4
GROUPS = 8
TOKENS_DEV = 512
HIDDEN = 512
DENSE_FF = 1024
EXPERT_FF = 256
EXPERTS = 64
TOP_K = 8
CAPACITY = 2 * TOKENS_DEV * TOP_K // EXPERTS
NORM_EPS = 1e-6


def rms_norm(values):
    return values * lax.rsqrt(jnp.mean(values * values, axis=-1, keepdims=True) + NORM_EPS)


def rms_back(values, grad_out):
    inv_rms = lax.rsqrt(jnp.mean(values * values, axis=-1, keepdims=True) + NORM_EPS)
    proj_mean = jnp.mean(grad_out * values, axis=-1, keepdims=True)
    return inv_rms * grad_out - values * (inv_rms * inv_rms * inv_rms) * proj_mean


def silu_grad(pre_act):
    sig_value = jax.nn.sigmoid(pre_act)
    return sig_value * (1.0 + pre_act * (1.0 - sig_value))


def draw_route(key):
    key_order, key_shift, key_perm = jax.random.split(key, 3)
    half_cap = CAPACITY // 2
    expert_order = jax.random.permutation(key_order, EXPERTS)
    pair_shift = jax.random.randint(key_shift, (EXPERTS // 2,), 0, half_cap + 1).at[0].set(half_cap)
    counts = jnp.full((EXPERTS,), half_cap, jnp.int32).at[expert_order[0::2]].add(pair_shift).at[expert_order[1::2]].add(-pair_shift)
    run_ends = jnp.cumsum(counts)
    positions = jnp.arange(TOKENS_DEV * TOP_K, dtype=jnp.int32)
    expert_ids = jnp.searchsorted(run_ends, positions, side='right')
    slot_ids = positions - (run_ends - counts)[expert_ids]
    route_table = (expert_ids * CAPACITY + slot_ids).astype(jnp.int32).reshape(TOP_K, TOKENS_DEV).T
    return route_table[jax.random.permutation(key_perm, TOKENS_DEV)]


def draw_routes(key):
    keys = jax.random.split(key, STAGES * 2 * GROUPS)
    return jax.vmap(draw_route)(keys).reshape(STAGES, 2, GROUPS * TOKENS_DEV, TOP_K)


def setup_inputs(seed: int = 0) -> dict:
    keys = jax.random.split(jax.random.key(seed), 12)
    tok_shape = (STAGES, GROUPS * TOKENS_DEV, HIDDEN)
    route_shape = (STAGES, 2, GROUPS * TOKENS_DEV, TOP_K)
    up_shape = (STAGES, 2, EXPERTS, HIDDEN, EXPERT_FF)
    down_shape = (STAGES, 2, EXPERTS, EXPERT_FF, HIDDEN)

    def normal_bf16(key, shape, scale):
        return (jax.random.normal(key, shape, jnp.float32) * scale).astype(jnp.bfloat16)

    def gate_draw(key):
        return (jax.random.uniform(key, route_shape, jnp.float32, 0.05, 1.95) * (2.0 * TOP_K ** -0.5)).astype(jnp.bfloat16)

    return dict(
        x_fwd=normal_bf16(keys[0], tok_shape, 1.0),
        x_bwd=normal_bf16(keys[1], tok_shape, 1.0),
        grad_in=normal_bf16(keys[2], tok_shape, 1.0),
        dense_in=normal_bf16(keys[3], (STAGES, 2, HIDDEN, DENSE_FF), HIDDEN ** -0.5),
        dense_out=normal_bf16(keys[4], (STAGES, 2, DENSE_FF, HIDDEN), DENSE_FF ** -0.5),
        exp_gate=normal_bf16(keys[5], up_shape, HIDDEN ** -0.5),
        exp_up=normal_bf16(keys[6], up_shape, HIDDEN ** -0.5),
        exp_down=normal_bf16(keys[7], down_shape, EXPERT_FF ** -0.5),
        route_fwd=draw_routes(keys[8]),
        gate_fwd=gate_draw(keys[9]),
        route_bwd=draw_routes(keys[10]),
        gate_bwd=gate_draw(keys[11]),
    )


def to_slots(rows, route):
    def one_source(src_rows, src_route):
        table = jnp.zeros((EXPERTS * CAPACITY, HIDDEN), src_rows.dtype)
        return table.at[src_route.reshape(-1)].set(src_rows.reshape(-1, HIDDEN))
    return jax.vmap(one_source)(rows, route).reshape(GROUPS, EXPERTS, CAPACITY, HIDDEN)


def from_slots(table, route):
    flat = table.reshape(GROUPS, EXPERTS * CAPACITY, HIDDEN)
    return jax.vmap(lambda src_table, src_route: src_table[src_route])(flat, route)


def dense_forward(tokens, w_in, w_out):
    normed = rms_norm(tokens.astype(jnp.float32)).astype(jnp.bfloat16)
    pre_act = jnp.dot(normed, w_in, preferred_element_type=jnp.float32)
    mid_act = jax.nn.silu(pre_act).astype(jnp.bfloat16)
    hidden = (tokens.astype(jnp.float32) + jnp.dot(mid_act, w_out, preferred_element_type=jnp.float32)).astype(jnp.bfloat16)
    return pre_act, hidden


def block_front(tokens, route, weights):
    w_in, w_out, w_gate, w_up, w_down = weights
    flat = tokens.reshape(GROUPS * TOKENS_DEV, HIDDEN)
    pre_act, hidden = dense_forward(flat, w_in, w_out)
    normed = rms_norm(hidden.astype(jnp.float32)).astype(jnp.bfloat16)
    spread = jnp.broadcast_to(normed.reshape(GROUPS, TOKENS_DEV, 1, HIDDEN), (GROUPS, TOKENS_DEV, TOP_K, HIDDEN))
    slots = to_slots(spread, route).astype(jnp.float32)
    gate_pre = jnp.einsum('gecd,edf->gecf', slots, w_gate.astype(jnp.float32))
    up_pre = jnp.einsum('gecd,edf->gecf', slots, w_up.astype(jnp.float32))
    expert_mid = (jax.nn.silu(gate_pre) * up_pre).astype(jnp.bfloat16)
    return flat, pre_act, hidden, slots, gate_pre, up_pre, expert_mid


def block_finish(saved, route, gate, weights):
    hidden = saved[2]
    expert_mid = saved[6]
    expert_out = jnp.einsum('gecf,efd->gecd', expert_mid.astype(jnp.float32), weights[4].astype(jnp.float32)).astype(jnp.bfloat16)
    picked = from_slots(expert_out, route)
    mixed = jnp.einsum('gtk,gtkd->gtd', gate.astype(jnp.float32), picked.astype(jnp.float32))
    return (hidden.reshape(GROUPS, TOKENS_DEV, HIDDEN).astype(jnp.float32) + mixed).astype(jnp.bfloat16)


def block_backward(grad_out, saved, route, gate, weights):
    w_in, w_out, w_gate, w_up, w_down = weights
    flat, pre_act, hidden, slots, gate_pre, up_pre, expert_mid = saved
    grad_send = (gate.astype(jnp.float32)[..., None] * grad_out.astype(jnp.float32)[:, :, None, :]).astype(jnp.bfloat16)
    grad_slots = to_slots(grad_send, route).astype(jnp.float32)
    grad_mid = jnp.einsum('gecd,efd->gecf', grad_slots, w_down.astype(jnp.float32))
    grad_gate_pre = (grad_mid * up_pre * silu_grad(gate_pre)).astype(jnp.bfloat16).astype(jnp.float32)
    grad_up_pre = (grad_mid * jax.nn.silu(gate_pre)).astype(jnp.bfloat16).astype(jnp.float32)
    dw_down = jnp.einsum('gecf,gecd->efd', expert_mid.astype(jnp.float32), grad_slots)
    dw_gate = jnp.einsum('gecd,gecf->edf', slots, grad_gate_pre)
    dw_up = jnp.einsum('gecd,gecf->edf', slots, grad_up_pre)
    grad_rows = (jnp.einsum('gecf,edf->gecd', grad_gate_pre, w_gate.astype(jnp.float32)) + jnp.einsum('gecf,edf->gecd', grad_up_pre, w_up.astype(jnp.float32))).astype(jnp.bfloat16)
    grad_norm = jnp.sum(from_slots(grad_rows, route).astype(jnp.float32), axis=2).reshape(GROUPS * TOKENS_DEV, HIDDEN)
    grad_hidden = grad_out.reshape(GROUPS * TOKENS_DEV, HIDDEN).astype(jnp.float32) + rms_back(hidden.astype(jnp.float32), grad_norm)
    grad_dense = jnp.dot(grad_hidden.astype(jnp.bfloat16), w_out.T, preferred_element_type=jnp.float32)
    grad_pre = (grad_dense * silu_grad(pre_act)).astype(jnp.bfloat16)
    grad_act = jnp.dot(grad_pre, w_in.T, preferred_element_type=jnp.float32)
    grad_tokens = (grad_hidden + rms_back(flat.astype(jnp.float32), grad_act)).astype(jnp.bfloat16)
    return grad_tokens.reshape(GROUPS, TOKENS_DEV, HIDDEN), dw_gate, dw_up, dw_down


def stage_step(operands):
    x_fwd, x_bwd, grad_in, dense_in, dense_out, exp_gate, exp_up, exp_down, route_fwd, gate_fwd, route_bwd, gate_bwd = operands
    tok_shape = (GROUPS, TOKENS_DEV, HIDDEN)
    route_shape = (2, GROUPS, TOKENS_DEV, TOP_K)
    route_f = route_fwd.reshape(route_shape)
    gate_f = gate_fwd.reshape(route_shape)
    route_b = route_bwd.reshape(route_shape)
    gate_b = gate_bwd.reshape(route_shape)
    weights = [(dense_in[block], dense_out[block], exp_gate[block], exp_up[block], exp_down[block]) for block in range(2)]
    tokens = x_fwd.reshape(tok_shape)
    for block in range(2):
        saved = block_front(tokens, route_f[block], weights[block])
        tokens = block_finish(saved, route_f[block], gate_f[block], weights[block])
    saved_first = block_front(x_bwd.reshape(tok_shape), route_b[0], weights[0])
    mid_tokens = block_finish(saved_first, route_b[0], gate_b[0], weights[0])
    saved_second = block_front(mid_tokens, route_b[1], weights[1])
    grad_mid, wg_two, wu_two, wd_two = block_backward(grad_in.reshape(tok_shape), saved_second, route_b[1], gate_b[1], weights[1])
    grad_first, wg_one, wu_one, wd_one = block_backward(grad_mid, saved_first, route_b[0], gate_b[0], weights[0])
    return (tokens.reshape(GROUPS * TOKENS_DEV, HIDDEN), grad_first.reshape(GROUPS * TOKENS_DEV, HIDDEN), jnp.stack([wg_one, wg_two]), jnp.stack([wu_one, wu_two]), jnp.stack([wd_one, wd_two]))


def reference(x_fwd, x_bwd, grad_in, dense_in, dense_out, exp_gate, exp_up, exp_down, route_fwd, gate_fwd, route_bwd, gate_bwd):
    results = lax.map(stage_step, (x_fwd, x_bwd, grad_in, dense_in, dense_out, exp_gate, exp_up, exp_down, route_fwd, gate_fwd, route_bwd, gate_bwd))
    y_out, dx_out, dw_gate, dw_up, dw_down = results
    return jnp.roll(y_out, 1, axis=0), jnp.roll(dx_out, -1, axis=0), dw_gate, dw_up, dw_down
```

```python
import functools

import jax
import jax.numpy as jnp
from jax import lax
from jax.experimental import pallas as pl
from jax.experimental.pallas import tpu as pltpu
from jax.sharding import PartitionSpec as P

NORM_EPS = 1e-6
F32 = jnp.float32
BF16 = jnp.bfloat16
VMEM = pl.BlockSpec(memory_space=pltpu.VMEM)
ANY = pl.BlockSpec(memory_space=pl.ANY)


def dot(a, b):
    return lax.dot_general(a, b, (((1,), (0,)), ((), ())), preferred_element_type=F32)


def dot_ta(a, b):
    return lax.dot_general(a, b, (((0,), (0,)), ((), ())), preferred_element_type=F32)


def dot_tb(a, b):
    return lax.dot_general(a, b, (((1,), (1,)), ((), ())), preferred_element_type=F32)


def rms_norm(v):
    return v * lax.rsqrt(jnp.mean(v * v, axis=-1, keepdims=True) + NORM_EPS)


def rms_back(v, g):
    inv = lax.rsqrt(jnp.mean(v * v, axis=-1, keepdims=True) + NORM_EPS)
    proj = jnp.mean(g * v, axis=-1, keepdims=True)
    return inv * g - v * (inv * inv * inv) * proj


def cost(flops, nbytes):
    return pl.CostEstimate(flops=int(flops), bytes_accessed=int(nbytes), transcendentals=0)


def params(mib=56):
    return pltpu.CompilerParams(vmem_limit_bytes=mib * 2**20)


ROWS = 128


def dense_fwd_body(x_ref, w1_ref, w2_ref, h_ref, z_ref, *p_ref):
    def step(i, _):
        rows = pl.ds(pl.multiple_of(i * ROWS, ROWS), ROWS)
        x = x_ref[rows, :].astype(F32)
        pre = dot(rms_norm(x).astype(BF16), w1_ref[...])
        if p_ref:
            p_ref[0][rows, :] = pre
        mid = (pre * jax.nn.sigmoid(pre)).astype(BF16)
        h = (x + dot(mid, w2_ref[...])).astype(BF16)
        h_ref[rows, :] = h
        z_ref[rows, :] = rms_norm(h.astype(F32)).astype(BF16)
        return 0
    lax.fori_loop(0, x_ref.shape[0] // ROWS, step, 0)


def dense_fwd(x, w1, w2, save):
    n, d = x.shape
    f = w1.shape[1]
    outs = [jax.ShapeDtypeStruct((n, d), BF16)] * 2
    if save:
        outs.append(jax.ShapeDtypeStruct((n, f), F32))
    return pl.pallas_call(
        dense_fwd_body, out_shape=outs, in_specs=[VMEM] * 3, out_specs=[VMEM] * len(outs),
        compiler_params=params(32), cost_estimate=cost(4 * n * d * f, 8 * n * d + 4 * d * f), name="dense_fwd")(x, w1, w2)


def dense_bwd_body(g_ref, dz_ref, h_ref, x_ref, p_ref, w1_ref, w2_ref, o_ref):
    def step(i, _):
        rows = pl.ds(pl.multiple_of(i * ROWS, ROWS), ROWS)
        dh = g_ref[rows, :].astype(F32) + rms_back(h_ref[rows, :].astype(F32), dz_ref[rows, :])
        pre = p_ref[rows, :]
        sig = jax.nn.sigmoid(pre)
        dp = (dot_tb(dh.astype(BF16), w2_ref[...]) * (sig * (1.0 + pre * (1.0 - sig)))).astype(BF16)
        da = dot_tb(dp, w1_ref[...])
        o_ref[rows, :] = (dh + rms_back(x_ref[rows, :].astype(F32), da)).astype(BF16)
        return 0
    lax.fori_loop(0, x_ref.shape[0] // ROWS, step, 0)


def dense_bwd(g, dz, h, x, p, w1, w2):
    n, d = x.shape
    f = w1.shape[1]
    return pl.pallas_call(
        dense_bwd_body, out_shape=jax.ShapeDtypeStruct((n, d), BF16), in_specs=[VMEM] * 7, out_specs=VMEM,
        compiler_params=params(32), cost_estimate=cost(4 * n * d * f, 16 * n * d + 4 * d * f), name="dense_bwd")(g, dz, h, x, p, w1, w2)


def table_body(route_ref, gate_ref, o_ref):
    n_pass, n_tok, top_k = route_ref.shape
    groups = o_ref.shape[0]
    n_exp = groups * o_ref.shape[3]
    lane = lax.broadcasted_iota(jnp.int32, (n_tok, 2 * n_exp), 1)
    first = lane < n_exp
    lane_exp = jnp.where(first, lane, lane - n_exp)
    ids = lax.broadcasted_iota(jnp.int32, (n_tok, 2 * n_exp), 0) + 1
    value = jnp.where(first, ids >> 4, ids & 15).astype(F32)
    slot = lax.broadcasted_iota(jnp.int32, (n_tok, 128), 1)

    def step(t, _):
        acc = jnp.zeros((4 * n_exp, 128), F32)
        for k in range(top_k):
            r = route_ref[t, :, k:k + 1]
            hit = (r >> 7) == lane_exp
            left = jnp.concatenate([jnp.where(hit, value, 0.0), jnp.where(hit & first, gate_ref[t, :, k:k + 1].astype(F32), 0.0)], axis=1)
            right = jnp.where((r & 127) == slot, 1.0, 0.0).astype(BF16)
            acc += dot_ta(left.astype(BF16), right)
        tok = acc[:n_exp] * 16.0 + acc[n_exp:2 * n_exp] - 1.0
        gat = acc[2 * n_exp:3 * n_exp]
        for g in range(groups):
            o_ref[g, t, 0] = tok[g * 8:(g + 1) * 8]
            o_ref[g, t, 1] = gat[g * 8:(g + 1) * 8]
        return 0
    lax.fori_loop(0, n_pass, step, 0)


def slot_tables(route, gate, groups):
    return pl.pallas_call(
        table_body, out_shape=jax.ShapeDtypeStruct((groups, route.shape[0], 2, 8, 128), F32), in_specs=[VMEM] * 2, out_specs=VMEM,
        compiler_params=params(32), cost_estimate=cost(1e9, 4e6), name="slot_tables")(route, gate)


MESH = pl.DeviceIdType.MESH
N_AG, N_RS = 8, 10


class Place:
    def __init__(self):
        me = lax.axis_index("ep")
        self.core, self.x, self.y = me % 2, (me // 2) % 2, me // 4
        self.pp = lax.axis_index("pp")
        self.near = {"c": me + 1 - 2 * self.core, "x": me + 2 - 4 * self.x, "y": me + 4 - 8 * self.y}

    def source(self, k, c):
        x, y = (self.x + k % 2) % 2, (self.y + k // 2) % 2
        core = self.core if c == 0 else 1 - self.core
        return y * 4 + x * 2 + core


def remote(place, src, dst, send, recv, to):
    return pltpu.make_async_remote_copy(src_ref=src, dst_ref=dst, send_sem=send, recv_sem=recv, device_id=(place.pp, place.near[to]), device_id_type=MESH)


def enter(place):
    barrier = pltpu.get_barrier_semaphore()
    for to in ("c", "x", "y"):
        pl.semaphore_signal(barrier, inc=1, device_id=(place.pp, place.near[to]), device_id_type=MESH)
    pl.semaphore_wait(barrier, 3)


class Rows:
    def __init__(self, place, slots, send, recv):
        h = slots.shape[2] // 2
        plan = ((0, 0, 1, 0, "x", None), (0, 0, 2, 0, "y", None), (0, 0, 0, 1, "c", None), (1, 0, 3, 0, "y", (0, h)), (1, 0, 1, 1, "c", None),
                (2, 0, 3, 0, "x", (h, h)), (2, 0, 2, 1, "c", None), (3, 0, 3, 1, "c", None))
        self.copies = []
        for i, (ks, cs, kd, cd, to, part) in enumerate(plan):
            s, d = slots.at[ks, cs], slots.at[kd, cd]
            if part is not None:
                s, d = s.at[pl.ds(*part)], d.at[pl.ds(*part)]
            self.copies.append(remote(place, s, d, send.at[i], recv.at[i], to))

    def start(self):
        for i in (0, 1, 2):
            self.copies[i].start()

    def pass_x(self):
        self.copies[0].wait_recv()
        self.copies[3].start()
        self.copies[4].start()

    def pass_y(self):
        self.copies[1].wait_recv()
        self.copies[5].start()
        self.copies[6].start()

    def pass_d(self):
        self.copies[3].wait_recv()
        self.copies[5].wait_recv()
        self.copies[7].start()

    def ready(self, k):
        self.copies[(2, 4, 6, 7)[k]].wait_recv()

    def drain(self):
        for c in self.copies:
            c.wait_send()


def add_rows(dst, a, b, lo, n):
    def step(i, _):
        rows = pl.ds(pl.multiple_of(lo + i * 64, 64), 64)
        dst[rows, :] = a[rows, :] + b[pl.ds(pl.multiple_of(lo - b_off(b, lo) + i * 64, 64), 64), :]
        return 0
    lax.fori_loop(0, n // 64, step, 0)


def b_off(b, lo):
    return lo if b.shape[0] <= lo or b.shape[0] < 512 else 0


class Sums:
    def __init__(self, place, mine, theirs, got, stage, send, recv):
        h = mine.shape[1] // 2
        self.h, self.mine, self.got, self.stage, self.recv, self.send = h, mine, got, stage, recv, send
        low, high = pl.ds(0, h), pl.ds(h, h)
        self.low, self.high = low, high
        n_buf = theirs.shape[0]
        self.theirs, self.n_buf, self.place = theirs, n_buf, place
        plan = ((1, low, "x"), (2, high, "y"), (3, low, "x"), (3, high, "y"), (2, low, "y"), (1, high, "x"))
        self.copies = [remote(place, mine.at[k].at[part], stage.at[i], send.at[4 + i], recv.at[4 + i], to) for i, (k, part, to) in enumerate(plan)]

    def pair(self, k):
        return remote(self.place, self.theirs.at[k % self.n_buf], self.got.at[k], self.send.at[k], self.recv.at[k], "c")

    def chip(self, k):
        self.pair(k).wait_recv()
        add_rows(self.mine.at[k], self.mine.at[k], self.got.at[k], 0, 2 * self.h)

    def chip_x(self):
        self.chip(1)
        self.copies[0].start()

    def chip_y(self):
        self.chip(2)
        self.copies[1].start()

    def chip_d(self):
        self.chip(3)
        self.copies[2].start()
        self.copies[3].start()

    def turn(self):
        h = self.h
        self.copies[2].wait_recv()
        add_rows(self.mine.at[2], self.mine.at[2], self.stage.at[2], 0, h)
        self.copies[4].start()
        self.copies[3].wait_recv()
        add_rows(self.mine.at[1], self.mine.at[1], self.stage.at[3], h, h)
        self.copies[5].start()

    def near(self):
        h = self.h
        self.copies[0].wait_recv()
        add_rows(self.mine.at[0], self.mine.at[0], self.stage.at[0], 0, h)
        self.copies[1].wait_recv()
        add_rows(self.mine.at[0], self.mine.at[0], self.stage.at[1], h, h)

    def finish(self, out, sem):
        h = self.h
        self.copies[4].wait_recv()
        add_rows(self.mine.at[0], self.mine.at[0], self.stage.at[4], 0, h)
        self.copies[5].wait_recv()
        add_rows(self.mine.at[0], self.mine.at[0], self.stage.at[5], h, h)
        done = pltpu.make_async_copy(self.mine.at[0], out, sem)
        done.start()
        for k in range(4 - self.n_buf, 4):
            self.pair(k).wait_send()
        for c in self.copies:
            c.wait_send()
        done.wait()


def slot_ids(n_tok, cap):
    return lax.broadcasted_iota(jnp.int32, (n_tok, cap), 0).astype(F32)


def one_hot(tab, src, t, e, ids):
    return jnp.where(tab[src, t, 0, pl.ds(e, 1), :] == ids, 1.0, 0.0).astype(BF16)


def gated(tab, src, t, e, ids):
    return jnp.where(tab[src, t, 0, pl.ds(e, 1), :] == ids, tab[src, t, 1, pl.ds(e, 1), :], 0.0).astype(BF16)


def pick(weights, rows):
    return dot_ta(jnp.concatenate(weights, axis=1), rows).astype(BF16)


def experts_fwd(place, tab, t, k, z, w, os, mine, theirs):
    n_exp, cap, n_tok = w[0].shape[0], tab.shape[4], z.shape[2]
    ids = slot_ids(n_tok, cap)
    src = [place.source(k, c) for c in range(2)]

    def step(i, _):
        es = (2 * i, 2 * i + 1)
        x = [pick([one_hot(tab, src[c], t, e, ids) for e in es], z[k, c]) for c in range(2)]
        for j, e in enumerate(es):
            xe = jnp.concatenate([x[c][j * cap:(j + 1) * cap] for c in range(2)], axis=0)
            a = dot(xe, w[0][e])
            b = dot(xe, w[1][e])
            o = dot((a * jax.nn.sigmoid(a) * b).astype(BF16), w[2][e]).astype(BF16)
            rows = pl.ds(pl.multiple_of(e * cap, cap), cap)
            os[0, rows, :] = o[:cap]
            os[1, rows, :] = o[cap:]
        return 0
    lax.fori_loop(0, n_exp // 2, step, 0)
    for c, p in ((1, theirs), (0, mine)):
        p[...] = dot(jnp.concatenate([gated(tab, src[c], t, e, ids) for e in range(n_exp)], axis=1), os[c])


def experts_bwd(place, tab, t, k, z, g, w, grads, os, mine, theirs):
    n_exp, cap, n_tok = w[0].shape[0], tab.shape[4], z.shape[2]
    ids = slot_ids(n_tok, cap)
    src = [place.source(k, c) for c in range(2)]

    def step(i, _):
        es = (2 * i, 2 * i + 1)
        x = [pick([one_hot(tab, src[c], t, e, ids) for e in es], z[k, c]) for c in range(2)]
        r = [pick([gated(tab, src[c], t, e, ids) for e in es], g[k, c]) for c in range(2)]
        for j, e in enumerate(es):
            xe = jnp.concatenate([x[c][j * cap:(j + 1) * cap] for c in range(2)], axis=0)
            re = jnp.concatenate([r[c][j * cap:(j + 1) * cap] for c in range(2)], axis=0)
            a = dot(xe, w[0][e])
            b = dot(xe, w[1][e])
            dm = dot_tb(re, w[2][e])
            sig = jax.nn.sigmoid(a)
            act = a * sig
            m = (act * b).astype(BF16)
            da = (dm * b * (sig * (1.0 + a * (1.0 - sig)))).astype(BF16)
            db = (dm * act).astype(BF16)
            o = (dot_tb(da, w[0][e]) + dot_tb(db, w[1][e])).astype(BF16)
            rows = pl.ds(pl.multiple_of(e * cap, cap), cap)
            os[0, rows, :] = o[:cap]
            os[1, rows, :] = o[cap:]
            grads[0][e] += dot_ta(xe, da)
            grads[1][e] += dot_ta(xe, db)
            grads[2][e] += dot_ta(m, re)
        return 0
    lax.fori_loop(0, n_exp // 2, step, 0)
    for c, p in ((1, theirs), (0, mine)):
        p[...] = dot(jnp.concatenate([one_hot(tab, src[c], t, e, ids) for e in range(n_exp)], axis=1), os[c])


def moe_body(kinds, tables, saved, n_in, n_out, *refs):
    ins, outs, scr = refs[:n_in], refs[n_in:n_in + n_out], list(refs[n_in + n_out:])
    tab, w_hbm, ins = ins[0], ins[1:4], list(ins[4:])
    outs = list(outs)
    w, os, load, store = scr[0:3], scr[3], scr[4], scr[5]
    scr = scr[6:]
    place = Place()
    copies = [pltpu.make_async_copy(a, b, load.at[i]) for i, (a, b) in enumerate(zip(w_hbm, w))]
    streams, first, grads = [], [], None
    for s, kind in enumerate(kinds):
        st = dict(kind=kind, t=tables[s])
        zs, send, recv = scr[:3]
        scr = scr[3:]
        st["z"] = zs
        st["zrows"] = None
        if kind == "again":
            first.append(pltpu.make_async_copy(ins.pop(0), zs, load.at[3 + 2 * s]))
        else:
            st["zrows"] = Rows(place, zs, send, recv)
            first.append(pltpu.make_async_copy(ins.pop(0), zs.at[0, 0], load.at[3 + 2 * s]))
        st["rows"] = [st["zrows"]] if st["zrows"] else []
        if kind != "fwd":
            gs, send, recv = scr[:3]
            scr = scr[3:]
            st["g"] = gs
            st["rows"].append(Rows(place, gs, send, recv))
            first.append(pltpu.make_async_copy(ins.pop(0), gs.at[0, 0], load.at[4 + 2 * s]))
            grads = scr[:3]
            scr = scr[3:]
        mine, theirs, got, stage, send, recv = scr[:6]
        scr = scr[6:]
        st["sums"] = Sums(place, mine, theirs, got, stage, send, recv)
        st["out"] = outs.pop(0)
        streams.append(st)
    for c in first:
        c.start()
    for c in copies:
        c.start()
    enter(place)
    for c in first:
        c.wait()
    for st in streams:
        for r in st["rows"]:
            r.start()
    if grads is not None:
        for gr in grads:
            def clear(e, _, gr=gr):
                gr[e] = jnp.zeros(gr.shape[1:], F32)
                return 0
            lax.fori_loop(0, gr.shape[0], clear, 0)
    for c in copies:
        c.wait()

    def run(st, k):
        sums = st["sums"]
        nb = sums.n_buf

        @pl.when(k >= nb)
        def _():
            sums.pair(k - nb).wait_send()
        theirs = sums.theirs.at[k % nb]
        if st["kind"] == "fwd":
            experts_fwd(place, tab, st["t"], k, st["z"], w, os, sums.mine.at[k], theirs)
        else:
            experts_bwd(place, tab, st["t"], k, st["z"], st["g"], w, grads, os, sums.mine.at[k], theirs)
        sums.pair(k).start()

    def before(st, k):
        for kk in range(4):
            @pl.when(k == kk)
            def _(kk=kk):
                for r in st["rows"]:
                    if kk == 1:
                        r.pass_x()
                        r.pass_y()
                    if kk == 3:
                        r.pass_d()
                    r.ready(kk)
                if kk == 3:
                    st["sums"].chip_x()

    def loop(k, _):
        for st in streams:
            before(st, k)
            run(st, k)
        return 0
    lax.fori_loop(0, 4, loop, 0)
    ends = []
    if grads is not None:
        for i, gr in enumerate(grads):
            ends.append(pltpu.make_async_copy(gr, outs[i], store.at[i]))
        outs = outs[3:]
    if saved:
        ends.append(pltpu.make_async_copy(streams[0]["z"], outs[0], store.at[3]))
    for c in ends:
        c.start()
    for st in streams:
        st["sums"].chip_y()
        st["sums"].chip_d()
    for st in streams:
        st["sums"].chip(0)
        st["sums"].near()
    for st in streams:
        st["sums"].turn()
    for i, st in enumerate(streams):
        st["sums"].finish(st["out"], store.at[4 + i])
        for r in st["rows"]:
            r.drain()
    for c in ends:
        c.wait()


def moe(kinds, tables, saved, tab, w, arrays, cid, n_buf):
    n, d = arrays[-1].shape
    n_exp, _, f = w[0].shape
    dma = pltpu.SemaphoreType.DMA
    ins = [tab, *w, *arrays]
    scratch = [pltpu.VMEM(a.shape, BF16) for a in w] + [pltpu.VMEM((2, n_exp * 128, d), BF16), dma((3 + 2 * len(kinds),)), dma((4 + len(kinds),))]
    outs = []
    for kind in kinds:
        scratch += [pltpu.VMEM((4, 2, n, d), BF16), dma((N_AG,)), dma((N_AG,))]
        if kind != "fwd":
            scratch += [pltpu.VMEM((4, 2, n, d), BF16), dma((N_AG,)), dma((N_AG,))]
            scratch += [pltpu.VMEM(a.shape, F32) for a in w]
        scratch += [pltpu.VMEM((4, n, d), F32), pltpu.VMEM((n_buf, n, d), F32), pltpu.VMEM((4, n, d), F32), pltpu.VMEM((6, n // 2, d), F32), dma((N_RS,)), dma((N_RS,))]
        outs.append(jax.ShapeDtypeStruct((n, d), F32))
    if any(k != "fwd" for k in kinds):
        outs += [jax.ShapeDtypeStruct(a.shape, F32) for a in w]
    if saved:
        outs.append(jax.ShapeDtypeStruct((4, 2, n, d), BF16))
    return pl.pallas_call(
        functools.partial(moe_body, kinds, tables, saved, len(ins), len(outs)), out_shape=outs,
        in_specs=[VMEM] + [ANY] * (len(ins) - 1), out_specs=[ANY] * len(outs), scratch_shapes=scratch,
        compiler_params=pltpu.CompilerParams(vmem_limit_bytes=67043328, collective_id=cid, has_side_effects=True),
        cost_estimate=cost(3e10, 5e7), name="moe_" + "_".join(kinds))(*ins)


def solution(mesh):
    groups = mesh.shape['ep']
    stages = mesh.shape['pp']
    to_next = [(sender, (sender + 1) % stages) for sender in range(stages)]
    to_prev = [(sender, (sender - 1) % stages) for sender in range(stages)]

    def local_step(x_fwd, x_bwd, grad_in, dense_in, dense_out, exp_gate, exp_up, exp_down, route_fwd, gate_fwd, route_bwd, gate_bwd):
        tab = slot_tables(jnp.concatenate([route_fwd[0], route_bwd[0]]), jnp.concatenate([gate_fwd[0], gate_bwd[0]]), groups)
        tab = lax.all_to_all(tab, 'ep', 0, 0, tiled=True)
        w1 = [dense_in[0, b] for b in range(2)]
        w2 = [dense_out[0, b] for b in range(2)]
        we = [(exp_gate[0, b], exp_up[0, b], exp_down[0, b]) for b in range(2)]

        def finish(h, mixed):
            return (h.astype(F32) + mixed).astype(BF16)

        h1, z1, p1 = dense_fwd(x_bwd[0], w1[0], w2[0], True)
        hf, zf = dense_fwd(x_fwd[0], w1[0], w2[0], False)
        mixed_b, mixed_f, z1_all = moe(("fwd", "fwd"), (2, 0), True, tab, we[0], (z1, zf), 0, 4)
        mid = finish(h1, mixed_b)
        h2, z2, p2 = dense_fwd(mid, w1[1], w2[1], True)
        hf, zf = dense_fwd(finish(hf, mixed_f), w1[1], w2[1], False)
        g2 = grad_in[0]
        dz2, mixed_f, *grads2 = moe(("bwd", "fwd"), (3, 1), False, tab, we[1], (z2, g2, zf), 1, 2)
        tokens = finish(hf, mixed_f)
        g1 = dense_bwd(g2, dz2, h2, mid, p2, w1[1], w2[1])
        dz1, *grads1 = moe(("again",), (2,), False, tab, we[0], (z1_all, g1), 2, 2)
        g0 = dense_bwd(g1, dz1, h1, x_bwd[0], p1, w1[0], w2[0])
        y_next = lax.ppermute(tokens, 'pp', to_next)
        dx_prev = lax.ppermute(g0, 'pp', to_prev)
        return (y_next[None], dx_prev[None]) + tuple(jnp.stack([a, b])[None] for a, b in zip(grads1, grads2))

    tok_spec = P('pp', 'ep', None)
    dense_spec = P('pp', None, None, None)
    exp_spec = P('pp', None, 'ep', None, None)
    route_spec = P('pp', None, 'ep', None)
    return jax.shard_map(local_step, mesh=mesh, in_specs=(tok_spec, tok_spec, tok_spec, dense_spec, dense_spec, exp_spec, exp_spec, exp_spec, route_spec, route_spec, route_spec, route_spec), out_specs=(tok_spec, tok_spec, exp_spec, exp_spec, exp_spec), check_vma=False)
```

```python
import functools

import jax
import jax.numpy as jnp
from jax import lax
from jax.experimental import pallas as pl
from jax.experimental.pallas import tpu as pltpu
from jax.sharding import PartitionSpec as P

NORM_EPS = 1e-6
F32 = jnp.float32
BF16 = jnp.bfloat16
VMEM = pl.BlockSpec(memory_space=pltpu.VMEM)
ANY = pl.BlockSpec(memory_space=pl.ANY)


def dot(a, b):
    return lax.dot_general(a, b, (((1,), (0,)), ((), ())), preferred_element_type=F32)


def dot_ta(a, b):
    return lax.dot_general(a, b, (((0,), (0,)), ((), ())), preferred_element_type=F32)


def dot_tb(a, b):
    return lax.dot_general(a, b, (((1,), (1,)), ((), ())), preferred_element_type=F32)


def rms_norm(v):
    return v * lax.rsqrt(jnp.mean(v * v, axis=-1, keepdims=True) + NORM_EPS)


def rms_back(v, g):
    inv = lax.rsqrt(jnp.mean(v * v, axis=-1, keepdims=True) + NORM_EPS)
    proj = jnp.mean(g * v, axis=-1, keepdims=True)
    return inv * g - v * (inv * inv * inv) * proj


def cost(flops, nbytes):
    return pl.CostEstimate(flops=int(flops), bytes_accessed=int(nbytes), transcendentals=0)


ROWS = 128


def dense_fwd(x_ref, w1, w2, h_ref, z_ref):
    def step(i, _):
        rows = pl.ds(pl.multiple_of(i * ROWS, ROWS), ROWS)
        x = x_ref[rows, :].astype(F32)
        pre = dot(rms_norm(x).astype(BF16), w1[...])
        mid = (pre * jax.nn.sigmoid(pre)).astype(BF16)
        h = (x + dot(mid, w2[...])).astype(BF16)
        h_ref[rows, :] = h
        z_ref[rows, :] = rms_norm(h.astype(F32)).astype(BF16)
        return 0
    lax.fori_loop(0, x_ref.shape[0] // ROWS, step, 0)


def dense_bwd(g_ref, dz_ref, h_ref, x_ref, w1, w2, o_ref):
    def step(i, _):
        rows = pl.ds(pl.multiple_of(i * ROWS, ROWS), ROWS)
        x = x_ref[rows, :].astype(F32)
        pre = dot(rms_norm(x).astype(BF16), w1[...])
        dh = g_ref[rows, :].astype(F32) + rms_back(h_ref[rows, :].astype(F32), dz_ref[rows, :])
        sig = jax.nn.sigmoid(pre)
        dp = (dot_tb(dh.astype(BF16), w2[...]) * (sig * (1.0 + pre * (1.0 - sig)))).astype(BF16)
        o_ref[rows, :] = (dh + rms_back(x, dot_tb(dp, w1[...]))).astype(BF16)
        return 0
    lax.fori_loop(0, x_ref.shape[0] // ROWS, step, 0)


def slot_tables(route_ref, gate_ref, o_ref, base):
    n_pass, n_tok, top_k = route_ref.shape
    groups = o_ref.shape[0]
    n_exp = groups * o_ref.shape[3]
    lane = lax.broadcasted_iota(jnp.int32, (n_tok, 2 * n_exp), 1)
    first = lane < n_exp
    lane_exp = jnp.where(first, lane, lane - n_exp)
    ids = lax.broadcasted_iota(jnp.int32, (n_tok, 2 * n_exp), 0) + 1
    value = jnp.where(first, ids >> 4, ids & 15).astype(F32)
    slot = lax.broadcasted_iota(jnp.int32, (n_tok, 128), 1)

    def step(t, _):
        acc = jnp.zeros((4 * n_exp, 128), F32)
        for k in range(top_k):
            r = route_ref[t, :, k:k + 1]
            hit = (r >> 7) == lane_exp
            left = jnp.concatenate([jnp.where(hit, value, 0.0), jnp.where(hit & first, gate_ref[t, :, k:k + 1].astype(F32), 0.0)], axis=1)
            right = jnp.where((r & 127) == slot, 1.0, 0.0).astype(BF16)
            acc += dot_ta(left.astype(BF16), right)
        tok = acc[:n_exp] * 16.0 + acc[n_exp:2 * n_exp] - 1.0
        gat = acc[2 * n_exp:3 * n_exp]
        for g in range(groups):
            o_ref[g, base + t, 0] = tok[g * 8:(g + 1) * 8]
            o_ref[g, base + t, 1] = gat[g * 8:(g + 1) * 8]
        return 0
    lax.fori_loop(0, n_pass, step, 0)


MESH = pl.DeviceIdType.MESH
N_AG, N_RS = 8, 10


class Place:
    def __init__(self):
        me = lax.axis_index("ep")
        self.core, self.x, self.y = me % 2, (me // 2) % 2, me // 4
        self.pp = lax.axis_index("pp")
        self.near = {"c": me + 1 - 2 * self.core, "x": me + 2 - 4 * self.x, "y": me + 4 - 8 * self.y}

    def source(self, k, c):
        x, y = (self.x + k % 2) % 2, (self.y + k // 2) % 2
        core = self.core if c == 0 else 1 - self.core
        return y * 4 + x * 2 + core


def remote(place, src, dst, send, recv, to):
    return pltpu.make_async_remote_copy(src_ref=src, dst_ref=dst, send_sem=send, recv_sem=recv, device_id=(place.pp, place.near[to]), device_id_type=MESH)


def greet(place, peers):
    for peer in peers:
        pl.semaphore_signal(pltpu.get_barrier_semaphore(), inc=1, device_id=(place.pp, peer), device_id_type=MESH)


def greeted(peers):
    pl.semaphore_wait(pltpu.get_barrier_semaphore(), len(peers))


class Rows:
    def __init__(self, place, slots, send, recv):
        h = slots.shape[2] // 2
        plan = ((0, 0, 1, 0, "x", None), (0, 0, 2, 0, "y", None), (0, 0, 0, 1, "c", None), (1, 0, 3, 0, "y", (0, h)), (1, 0, 1, 1, "c", None),
                (2, 0, 3, 0, "x", (h, h)), (2, 0, 2, 1, "c", None), (3, 0, 3, 1, "c", None))
        self.copies = []
        for i, (ks, cs, kd, cd, to, part) in enumerate(plan):
            s, d = slots.at[ks, cs], slots.at[kd, cd]
            if part is not None:
                s, d = s.at[pl.ds(*part)], d.at[pl.ds(*part)]
            self.copies.append(remote(place, s, d, send.at[i], recv.at[i], to))

    def start(self):
        for i in (0, 1, 2):
            self.copies[i].start()

    def pass_x(self):
        self.copies[0].wait_recv()
        self.copies[3].start()
        self.copies[4].start()

    def pass_y(self):
        self.copies[1].wait_recv()
        self.copies[5].start()
        self.copies[6].start()

    def pass_d(self):
        self.copies[3].wait_recv()
        self.copies[5].wait_recv()
        self.copies[7].start()

    def ready(self, k):
        self.copies[(2, 4, 6, 7)[k]].wait_recv()

    def drain(self):
        for c in self.copies:
            c.wait_send()


def add_rows(dst, b, lo, n):
    def step(i, _):
        at = pl.multiple_of(i * 64, 64)
        rows = pl.ds(lo + at, 64)
        dst[rows, :] = dst[rows, :] + b[pl.ds(at, 64), :]
        return 0
    lax.fori_loop(0, n // 64, step, 0)


class Sums:
    def __init__(self, place, mine, theirs, got, stage, send, recv):
        h = mine.shape[1] // 2
        self.h, self.mine, self.got, self.stage, self.recv, self.send = h, mine, got, stage, recv, send
        low, high = pl.ds(0, h), pl.ds(h, h)
        self.low, self.high = low, high
        n_buf = theirs.shape[0]
        self.theirs, self.n_buf, self.place = theirs, n_buf, place
        plan = ((1, low, "x"), (2, high, "y"), (3, low, "x"), (3, high, "y"), (2, low, "y"), (1, high, "x"))
        self.copies = [remote(place, mine.at[k].at[part], stage.at[i], send.at[4 + i], recv.at[4 + i], to) for i, (k, part, to) in enumerate(plan)]

    def pair(self, k):
        return remote(self.place, self.theirs.at[k % self.n_buf], self.got.at[k], self.send.at[k], self.recv.at[k], "c")

    def chip(self, k):
        self.pair(k).wait_recv()
        add_rows(self.mine.at[k], self.got.at[k], 0, 2 * self.h)

    def chip_x(self):
        self.chip(1)
        self.copies[0].start()

    def chip_y(self):
        self.chip(2)
        self.copies[1].start()

    def chip_d(self):
        self.chip(3)
        self.copies[2].start()
        self.copies[3].start()

    def turn(self):
        h = self.h
        self.copies[2].wait_recv()
        add_rows(self.mine.at[2], self.stage.at[2], 0, h)
        self.copies[4].start()
        self.copies[3].wait_recv()
        add_rows(self.mine.at[1], self.stage.at[3], h, h)
        self.copies[5].start()

    def near(self):
        h = self.h
        self.copies[0].wait_recv()
        add_rows(self.mine.at[0], self.stage.at[0], 0, h)
        self.copies[1].wait_recv()
        add_rows(self.mine.at[0], self.stage.at[1], h, h)

    def last(self):
        h = self.h
        self.copies[4].wait_recv()
        add_rows(self.mine.at[0], self.stage.at[4], 0, h)
        self.copies[5].wait_recv()
        add_rows(self.mine.at[0], self.stage.at[5], h, h)

    def drain(self, last):
        if last:
            for k in range(4 - self.n_buf, 4):
                self.pair(k).wait_send()
        for c in self.copies:
            c.wait_send()


def slot_ids(n_tok, cap):
    return lax.broadcasted_iota(jnp.int32, (n_tok, cap), 0).astype(F32)


def one_hot(tab, src, t, e, ids):
    return jnp.where(tab[src, t, 0, pl.ds(e, 1), :] == ids, 1.0, 0.0).astype(BF16)


def gated(tab, src, t, e, ids):
    return jnp.where(tab[src, t, 0, pl.ds(e, 1), :] == ids, tab[src, t, 1, pl.ds(e, 1), :], 0.0).astype(BF16)


def pick(weights, rows):
    return dot_ta(jnp.concatenate(weights, axis=1), rows).astype(BF16)


def experts_fwd(place, tab, t, k, z, w, os, mine, theirs):
    n_exp, cap, n_tok = w[0].shape[0], tab.shape[4], z.shape[2]
    ids = slot_ids(n_tok, cap)
    src = [place.source(k, c) for c in range(2)]

    def step(i, _):
        es = (2 * i, 2 * i + 1)
        x = [pick([one_hot(tab, src[c], t, e, ids) for e in es], z[k, c]) for c in range(2)]
        for j, e in enumerate(es):
            xe = jnp.concatenate([x[c][j * cap:(j + 1) * cap] for c in range(2)], axis=0)
            a = dot(xe, w[0][e])
            b = dot(xe, w[1][e])
            o = dot((a * jax.nn.sigmoid(a) * b).astype(BF16), w[2][e]).astype(BF16)
            rows = pl.ds(pl.multiple_of(e * cap, cap), cap)
            os[0, rows, :] = o[:cap]
            os[1, rows, :] = o[cap:]
        return 0
    lax.fori_loop(0, n_exp // 2, step, 0)
    for c, p in ((1, theirs), (0, mine)):
        p[...] = dot(jnp.concatenate([gated(tab, src[c], t, e, ids) for e in range(n_exp)], axis=1), os[c])


def experts_bwd(place, tab, t, k, z, g, w, grads, os, mine, theirs):
    n_exp, cap, n_tok = w[0].shape[0], tab.shape[4], z.shape[2]
    ids = slot_ids(n_tok, cap)
    src = [place.source(k, c) for c in range(2)]

    def step(i, _):
        es = (2 * i, 2 * i + 1)
        x = [pick([one_hot(tab, src[c], t, e, ids) for e in es], z[k, c]) for c in range(2)]
        r = [pick([gated(tab, src[c], t, e, ids) for e in es], g[k, c]) for c in range(2)]
        for j, e in enumerate(es):
            xe = jnp.concatenate([x[c][j * cap:(j + 1) * cap] for c in range(2)], axis=0)
            re = jnp.concatenate([r[c][j * cap:(j + 1) * cap] for c in range(2)], axis=0)
            a = dot(xe, w[0][e])
            b = dot(xe, w[1][e])
            dm = dot_tb(re, w[2][e])
            sig = jax.nn.sigmoid(a)
            act = a * sig
            m = (act * b).astype(BF16)
            da = (dm * b * (sig * (1.0 + a * (1.0 - sig)))).astype(BF16)
            db = (dm * act).astype(BF16)
            o = (dot_tb(da, w[0][e]) + dot_tb(db, w[1][e])).astype(BF16)
            rows = pl.ds(pl.multiple_of(e * cap, cap), cap)
            os[0, rows, :] = o[:cap]
            os[1, rows, :] = o[cap:]
            grads[0][e] += dot_ta(xe, da)
            grads[1][e] += dot_ta(xe, db)
            grads[2][e] += dot_ta(m, re)
        return 0
    lax.fori_loop(0, n_exp // 2, step, 0)
    for c, p in ((1, theirs), (0, mine)):
        p[...] = dot(jnp.concatenate([one_hot(tab, src[c], t, e, ids) for e in range(n_exp)], axis=1), os[c])


def add_hidden(h_ref, mixed):
    def step(i, _):
        rows = pl.ds(pl.multiple_of(i * ROWS, ROWS), ROWS)
        h_ref[rows, :] = (h_ref[rows, :].astype(F32) + mixed[rows, :]).astype(BF16)
        return 0
    lax.fori_loop(0, h_ref.shape[0] // ROWS, step, 0)


class Names:
    def __init__(self, names, refs):
        self.by = dict(zip(names, refs))

    def __call__(self, name):
        return self.by.get(name)


def moe_body(kinds, passes, block, names, *refs):
    ref = Names(names, refs)
    place = Place()
    load, store = ref("load"), ref("store")
    n_load, n_store = [0], [0]

    def fetch(a, b):
        n_load[0] += 1
        c = pltpu.make_async_copy(a, b, load.at[n_load[0] - 1])
        c.start()
        return c

    def put(a, b):
        n_store[0] += 1
        c = pltpu.make_async_copy(a, b, store.at[n_store[0] - 1])
        c.start()
        return c

    first_phase = ref("tab_out") is not None
    peers = [place.source(j // 2, j % 2) for j in range(1, 8)] if first_phase else list(place.near.values())
    greet(place, peers)

    streams = []
    for s, kind in enumerate(kinds):
        st = dict(kind=kind, t=passes[s], z=ref(f"z{s}"), h=ref(f"h{s}"), x=ref(f"x{s}"), g=ref(f"g{s}"))
        st["rows"] = []
        if kind != "again":
            st["rows"].append(Rows(place, st["z"], ref(f"z{s}_send"), ref(f"z{s}_recv")))
        if kind != "fwd":
            st["rows"].append(Rows(place, st["g"], ref(f"g{s}_send"), ref(f"g{s}_recv")))
        st["sums"] = Sums(place, ref(f"mine{s}"), ref("theirs"), ref(f"got{s}"), ref(f"stage{s}"), ref(f"s{s}_send"), ref(f"s{s}_recv"))
        x_in = st["x"] if st["x"] is not None else st["z"].at[0, 0]
        st["x_in"] = x_in
        st["loads"] = []
        if kind == "again":
            st["loads"].append(fetch(ref(f"g{s}_in"), st["g"].at[0, 0]))
        st["loads"].append(fetch(ref(f"x{s}_in"), x_in))
        st["later"] = []
        streams.append(st)
    dense = [fetch(ref(n + "_in").at[0, block], ref(n)) for n in ("w1", "w2")]
    for s, st in enumerate(streams):
        if st["kind"] == "bwd":
            st["later"].append(fetch(ref(f"g{s}_in"), st["g"].at[0, 0]))
        if st["kind"] == "again":
            st["later"].append(fetch(ref(f"z{s}_in"), st["z"]))
            st["later"].append(fetch(ref(f"h{s}_in"), st["h"]))
    w = [ref(n) for n in ("wg", "wu", "wd")]
    experts = [fetch(ref(n + "_in").at[0, block], v) for n, v in zip(("wg", "wu", "wd"), w)]
    grads = [ref(n) for n in ("dg", "du", "dd")] if ref("dg") is not None else None
    tab, os = ref("tab"), ref("os")
    w1, w2 = ref("w1"), ref("w2")

    for c in dense:
        c.wait()
    greeted_yet = False
    for s, st in enumerate(streams):
        for c in st["loads"]:
            c.wait()
        if st["kind"] != "again":
            dense_fwd(st["x_in"], w1, w2, st["h"], st["z"].at[0, 0])
        if not greeted_yet:
            greeted(peers)
            greeted_yet = True
        for c in st["later"]:
            c.wait()
        for r in st["rows"]:
            r.start()
    ends = []
    if first_phase:
        mail = ref("mail")
        slot_tables(ref("route_fwd"), ref("gate_fwd"), mail, 0)
        slot_tables(ref("route_bwd"), ref("gate_bwd"), mail, 2)
        me = place.source(0, 0)
        own = fetch(mail.at[me], tab.at[me])
        post = [pltpu.make_async_remote_copy(src_ref=mail.at[to], dst_ref=tab.at[me], send_sem=ref("t_send").at[j], recv_sem=ref("t_recv").at[j],
                                             device_id=(place.pp, to), device_id_type=MESH) for j, to in enumerate(peers)]
        for c in post:
            c.start()
        own.wait()
        for c in post:
            c.wait_recv()
        ends.append(put(tab, ref("tab_out")))
    if grads is not None:
        for gr in grads:
            def clear(e, _, gr=gr):
                gr[e] = jnp.zeros(gr.shape[1:], F32)
                return 0
            lax.fori_loop(0, gr.shape[0], clear, 0)
    for c in experts:
        c.wait()

    def unit(st, k):
        sums = st["sums"]
        nb = sums.n_buf

        @pl.when(k >= nb)
        def _():
            sums.pair(k - nb).wait_send()
        if st is not a:
            @pl.when(k < nb)
            def _():
                a["sums"].pair(k + 4 - nb).wait_send()
        theirs = sums.theirs.at[k % nb]
        if st["kind"] == "fwd":
            experts_fwd(place, tab, st["t"], k, st["z"], w, os, sums.mine.at[k], theirs)
        else:
            experts_bwd(place, tab, st["t"], k, st["z"], st["g"], w, grads, os, sums.mine.at[k], theirs)
        sums.pair(k).start()

    def pass_xy(st):
        for r in st["rows"]:
            r.pass_x()
            r.pass_y()

    def pass_d(st):
        for r in st["rows"]:
            r.pass_d()

    def ready(st, k):
        for r in st["rows"]:
            r.ready(k)

    a, b = streams[0], streams[-1]
    two = len(streams) == 2
    before = {(0, 1): [lambda: pass_xy(a)], (0, 3): [lambda: pass_d(a)]}
    after = {(0, 2): [a["sums"].chip_x], (0, 3): [a["sums"].chip_y]}
    if two:
        before[0, 2] = [lambda: pass_xy(b)] if a["kind"] == "fwd" else []
        if a["kind"] != "fwd":
            before[0, 3].append(lambda: pass_xy(b))
        before[1, 0] = [lambda: pass_d(b)]
        after[1, 0] = [a["sums"].chip_d]
        after[1, 1] = [lambda: a["sums"].chip(0)]
        after[1, 2] = [b["sums"].chip_x, a["sums"].turn]
        after[1, 3] = [b["sums"].chip_y]
    for s, st in enumerate(streams):
        def loop(k, _, s=s, st=st):
            for kk in range(4):
                @pl.when(k == kk)
                def _(kk=kk):
                    for f in before.get((s, kk), []):
                        f()
                    ready(st, kk)
            unit(st, k)
            for kk in range(4):
                if (s, kk) in after:
                    @pl.when(k == kk)
                    def _(kk=kk):
                        for f in after[s, kk]:
                            f()
            return 0
        lax.fori_loop(0, 4, loop, 0)
    if grads is not None:
        ends += [put(gr, ref(n + "_out")) for gr, n in zip(grads, ("dg", "du", "dd"))]
    if first_phase:
        ends.append(put(a["z"], ref("z0_out")))
    b["sums"].chip_d()
    if two:
        a["sums"].near()
    b["sums"].chip(0)
    if two:
        finish(a, 0, ref, w1, w2, put, ends, False)
    b["sums"].turn()
    b["sums"].near()
    finish(b, len(streams) - 1, ref, w1, w2, put, ends, True)
    if first_phase:
        for c in post:
            c.wait_send()
    for c in ends:
        c.wait()


def finish(st, s, ref, w1, w2, put, ends, last):
    sums = st["sums"]
    sums.last()
    if st["kind"] == "fwd":
        if ref(f"h{s}_out") is not None:
            keep = put(st["h"], ref(f"h{s}_out"))
            keep.wait()
        add_hidden(st["h"], sums.mine.at[0])
        ends.append(put(st["h"], ref(f"y{s}_out")))
    else:
        if ref(f"h{s}_out") is not None:
            ends.append(put(st["h"], ref(f"h{s}_out")))
        dense_bwd(st["g"].at[0, 0], sums.mine.at[0], st["h"], st["x"], w1, w2, st["x"])
        ends.append(put(st["x"], ref(f"y{s}_out")))
    sums.drain(last)
    for r in st["rows"]:
        r.drain()


def moe(kinds, passes, block, ins, out_names, weights, cid, n_buf):
    n, d = 512, 512
    dma = pltpu.SemaphoreType.DMA
    ins = dict(ins)
    ins.update(zip(("wg_in", "wu_in", "wd_in", "w1_in", "w2_in"), weights))
    shapes = [x.shape[2:] for x in weights]
    n_exp = shapes[0][0]
    groups = 8
    tab_shape = (groups, 4, 2, 8, 128)
    row = jax.ShapeDtypeStruct((n, d), BF16)
    made = {"tab_out": jax.ShapeDtypeStruct(tab_shape, F32), "z0_out": jax.ShapeDtypeStruct((4, 2, n, d), BF16)}
    made.update({nm + "_out": jax.ShapeDtypeStruct(sh, F32) for nm, sh in zip(("dg", "du", "dd"), shapes)})
    outs = {nm: made.get(nm, row) for nm in out_names}
    scratch = {nm: pltpu.VMEM(sh, BF16) for nm, sh in zip(("wg", "wu", "wd", "w1", "w2"), shapes)}
    scratch.update(os=pltpu.VMEM((2, n_exp * 128, d), BF16), theirs=pltpu.VMEM((n_buf, n, d), F32), load=dma((16,)), store=dma((12,)))
    if "tab_out" in outs:
        scratch.update(tab=pltpu.VMEM(tab_shape, F32), mail=pltpu.VMEM(tab_shape, F32), t_send=dma((7,)), t_recv=dma((7,)))
    slots = pltpu.VMEM((4, 2, n, d), BF16)
    for s, kind in enumerate(kinds):
        scratch[f"z{s}"] = slots
        scratch[f"h{s}"] = pltpu.VMEM((n, d), BF16)
        if kind != "again":
            scratch.update({f"z{s}_send": dma((N_AG,)), f"z{s}_recv": dma((N_AG,))})
        if kind != "fwd":
            scratch.update({f"g{s}": slots, f"x{s}": pltpu.VMEM((n, d), BF16), f"g{s}_send": dma((N_AG,)), f"g{s}_recv": dma((N_AG,))})
            scratch.update({nm: pltpu.VMEM(sh, F32) for nm, sh in zip(("dg", "du", "dd"), shapes)})
        scratch.update({f"mine{s}": pltpu.VMEM((4, n, d), F32), f"got{s}": pltpu.VMEM((4, n, d), F32),
                        f"stage{s}": pltpu.VMEM((6, n // 2, d), F32), f"s{s}_send": dma((N_RS,)), f"s{s}_recv": dma((N_RS,))})
    small = ("tab", "route_fwd", "route_bwd", "gate_fwd", "gate_bwd")
    res = pl.pallas_call(
        functools.partial(moe_body, kinds, passes, block, list(ins) + list(outs) + list(scratch)), out_shape=list(outs.values()),
        in_specs=[VMEM if nm in small else ANY for nm in ins], out_specs=[ANY] * len(outs), scratch_shapes=list(scratch.values()),
        compiler_params=pltpu.CompilerParams(vmem_limit_bytes=67043328, collective_id=cid, has_side_effects=True),
        cost_estimate=cost(3e10, 5e7), name="moe_" + "_".join(kinds))(*ins.values())
    return dict(zip(outs, res))


def solution(mesh):
    stages = mesh.shape['pp']
    to_next = [(sender, (sender + 1) % stages) for sender in range(stages)]
    to_prev = [(sender, (sender - 1) % stages) for sender in range(stages)]

    def local_step(x_fwd, x_bwd, grad_in, dense_in, dense_out, exp_gate, exp_up, exp_down, route_fwd, gate_fwd, route_bwd, gate_bwd):
        weights = (exp_gate, exp_up, exp_down, dense_in, dense_out)
        route = dict(route_fwd=route_fwd[0], route_bwd=route_bwd[0], gate_fwd=gate_fwd[0], gate_bwd=gate_bwd[0])
        grads = ("dg_out", "du_out", "dd_out")
        one = moe(("fwd", "fwd"), (2, 0), 0, dict(route, x0_in=x_bwd[0], x1_in=x_fwd[0]), ("y0_out", "y1_out", "h0_out", "tab_out", "z0_out"), weights, 0, 2)
        two = moe(("bwd", "fwd"), (3, 1), 1, dict(tab=one["tab_out"], x0_in=one["y0_out"], g0_in=grad_in[0], x1_in=one["y1_out"]), ("y0_out", "y1_out") + grads, weights, 1, 2)
        three = moe(("again",), (2,), 0, dict(tab=one["tab_out"], x0_in=x_bwd[0], h0_in=one["h0_out"], z0_in=one["z0_out"], g0_in=two["y0_out"]), ("y0_out",) + grads, weights, 2, 2)
        y_next = lax.ppermute(two["y1_out"], 'pp', to_next)
        dx_prev = lax.ppermute(three["y0_out"], 'pp', to_prev)
        return (y_next[None], dx_prev[None]) + tuple(jnp.stack([three[g], two[g]])[None] for g in grads)

    tok_spec = P('pp', 'ep', None)
    dense_spec = P('pp', None, None, None)
    exp_spec = P('pp', None, 'ep', None, None)
    route_spec = P('pp', None, 'ep', None)
    return jax.shard_map(local_step, mesh=mesh, in_specs=(tok_spec, tok_spec, tok_spec, dense_spec, dense_spec, exp_spec, exp_spec, exp_spec, route_spec, route_spec, route_spec, route_spec), out_specs=(tok_spec, tok_spec, exp_spec, exp_spec, exp_spec), check_vma=False)
```

```python
import functools

import jax
import jax.numpy as jnp
from jax import lax
from jax.experimental import pallas as pl
from jax.experimental.pallas import tpu as pltpu
from jax.sharding import PartitionSpec as P

NORM_EPS = 1e-6
F32 = jnp.float32
BF16 = jnp.bfloat16
VMEM = pl.BlockSpec(memory_space=pltpu.VMEM)
ANY = pl.BlockSpec(memory_space=pl.ANY)


def dot(a, b):
    return lax.dot_general(a, b, (((1,), (0,)), ((), ())), preferred_element_type=F32)


def dot_ta(a, b):
    return lax.dot_general(a, b, (((0,), (0,)), ((), ())), preferred_element_type=F32)


def dot_tb(a, b):
    return lax.dot_general(a, b, (((1,), (1,)), ((), ())), preferred_element_type=F32)


def rms_norm(v):
    return v * lax.rsqrt(jnp.mean(v * v, axis=-1, keepdims=True) + NORM_EPS)


def rms_back(v, g):
    inv = lax.rsqrt(jnp.mean(v * v, axis=-1, keepdims=True) + NORM_EPS)
    proj = jnp.mean(g * v, axis=-1, keepdims=True)
    return inv * g - v * (inv * inv * inv) * proj


def cost(flops, nbytes):
    return pl.CostEstimate(flops=int(flops), bytes_accessed=int(nbytes), transcendentals=0)


ROWS = 256


def dense_fwd(x_ref, w1, w2, h_ref, z_ref):
    def step(i, _):
        rows = pl.ds(pl.multiple_of(i * ROWS, ROWS), ROWS)
        x = x_ref[rows, :].astype(F32)
        pre = dot(rms_norm(x).astype(BF16), w1[...])
        mid = (pre * jax.nn.sigmoid(pre)).astype(BF16)
        h = (x + dot(mid, w2[...])).astype(BF16)
        h_ref[rows, :] = h
        z_ref[rows, :] = rms_norm(h.astype(F32)).astype(BF16)
        return 0
    lax.fori_loop(0, x_ref.shape[0] // ROWS, step, 0)


def dense_slope(x_ref, w1, slope):
    half = slope.shape[2]

    def step(i, _):
        rows = pl.ds(pl.multiple_of(i * ROWS, ROWS), ROWS)
        pre = dot(rms_norm(x_ref[rows, :].astype(F32)).astype(BF16), w1[...])
        sig = jax.nn.sigmoid(pre)
        val = sig * (1.0 + pre * (1.0 - sig))
        slope[0, rows, :] = val[:, :half]
        slope[1, rows, :] = val[:, half:]
        return 0
    lax.fori_loop(0, x_ref.shape[0] // ROWS, step, 0)


def dense_bwd(g_ref, dz_ref, h_ref, x_ref, slope, w1, w2, o_ref):
    def step(i, _):
        rows = pl.ds(pl.multiple_of(i * ROWS, ROWS), ROWS)
        x = x_ref[rows, :].astype(F32)
        dh = g_ref[rows, :].astype(F32) + rms_back(h_ref[rows, :].astype(F32), dz_ref[rows, :])
        turned = jnp.concatenate([slope[0, rows, :], slope[1, rows, :]], axis=1)
        dp = (dot_tb(dh.astype(BF16), w2[...]) * turned).astype(BF16)
        o_ref[rows, :] = (dh + rms_back(x, dot_tb(dp, w1[...]))).astype(BF16)
        return 0
    lax.fori_loop(0, x_ref.shape[0] // ROWS, step, 0)


def slot_tables(route_ref, gate_ref, o_ref, base):
    n_pass, top_k, n_tok = route_ref.shape
    groups = o_ref.shape[0]
    n_exp = groups * o_ref.shape[3]
    row = lax.broadcasted_iota(jnp.int32, (2 * n_exp, n_tok), 0)
    first = row < n_exp
    row_exp = jnp.where(first, row, row - n_exp)
    ids = lax.broadcasted_iota(jnp.int32, (2 * n_exp, n_tok), 1) + 1
    value = jnp.where(first, ids >> 4, ids & 15).astype(F32)
    slot = lax.broadcasted_iota(jnp.int32, (128, n_tok), 0)

    def step(t, _):
        acc = jnp.zeros((3 * n_exp, 128), F32)
        for k in range(top_k):
            r = route_ref[t, k:k + 1, :]
            hit = (r >> 7) == row_exp
            left = jnp.concatenate([jnp.where(hit, value, 0.0), jnp.where(hit[:n_exp], gate_ref[t, k:k + 1, :].astype(F32), 0.0)], axis=0)
            right = jnp.where((r & 127) == slot, 1.0, 0.0).astype(BF16)
            acc += dot_tb(left.astype(BF16), right)
        tok = acc[:n_exp] * 16.0 + acc[n_exp:2 * n_exp] - 1.0
        gat = acc[2 * n_exp:]
        for g in range(groups):
            o_ref[g, base + t, 0] = tok[g * 8:(g + 1) * 8]
            o_ref[g, base + t, 1] = gat[g * 8:(g + 1) * 8]
        return 0
    lax.fori_loop(0, n_pass, step, 0)


MESH = pl.DeviceIdType.MESH
N_AG, N_RS = 8, 10


class Place:
    def __init__(self):
        me = lax.axis_index("ep")
        self.core, self.x, self.y = me % 2, (me // 2) % 2, me // 4
        self.pp = lax.axis_index("pp")
        self.near = {"c": me + 1 - 2 * self.core, "x": me + 2 - 4 * self.x, "y": me + 4 - 8 * self.y}

    def source(self, k, c):
        x, y = (self.x + k % 2) % 2, (self.y + k // 2) % 2
        core = self.core if c == 0 else 1 - self.core
        return y * 4 + x * 2 + core


def remote(place, src, dst, send, recv, to):
    return pltpu.make_async_remote_copy(src_ref=src, dst_ref=dst, send_sem=send, recv_sem=recv, device_id=(place.pp, place.near[to]), device_id_type=MESH)


def greet(place, peers):
    for peer in peers:
        pl.semaphore_signal(pltpu.get_barrier_semaphore(), inc=1, device_id=(place.pp, peer), device_id_type=MESH)


def greeted(peers):
    pl.semaphore_wait(pltpu.get_barrier_semaphore(), len(peers))


class Rows:
    def __init__(self, place, slots, send, recv):
        h = slots.shape[2] // 2
        plan = ((0, 0, 1, 0, "x", None), (0, 0, 2, 0, "y", None), (0, 0, 0, 1, "c", None), (1, 0, 3, 0, "y", (0, h)), (1, 0, 1, 1, "c", None),
                (2, 0, 3, 0, "x", (h, h)), (2, 0, 2, 1, "c", None), (3, 0, 3, 1, "c", None))
        self.copies = []
        for i, (ks, cs, kd, cd, to, part) in enumerate(plan):
            s, d = slots.at[ks, cs], slots.at[kd, cd]
            if part is not None:
                s, d = s.at[pl.ds(*part)], d.at[pl.ds(*part)]
            self.copies.append(remote(place, s, d, send.at[i], recv.at[i], to))

    def start(self):
        for i in (0, 1, 2):
            self.copies[i].start()

    def pass_x(self):
        self.copies[0].wait_recv()
        self.copies[3].start()
        self.copies[4].start()

    def pass_y(self):
        self.copies[1].wait_recv()
        self.copies[5].start()
        self.copies[6].start()

    def pass_d(self):
        self.copies[3].wait_recv()
        self.copies[5].wait_recv()
        self.copies[7].start()

    def ready(self, k):
        self.copies[(2, 4, 6, 7)[k]].wait_recv()

    def drain(self):
        for c in self.copies:
            c.wait_send()


def add_rows(dst, b, lo, n):
    def step(i, _):
        at = pl.multiple_of(i * 64, 64)
        rows = pl.ds(lo + at, 64)
        dst[rows, :] = dst[rows, :] + b[pl.ds(at, 64), :]
        return 0
    lax.fori_loop(0, n // 64, step, 0)


class Sums:
    def __init__(self, place, mine, theirs, got, stage, send, recv):
        h = mine.shape[1] // 2
        self.h, self.mine, self.got, self.stage, self.recv, self.send = h, mine, got, stage, recv, send
        low, high = pl.ds(0, h), pl.ds(h, h)
        self.low, self.high = low, high
        n_buf = theirs.shape[0]
        self.theirs, self.n_buf, self.place = theirs, n_buf, place
        plan = ((1, low, "x"), (2, high, "y"), (3, low, "x"), (3, high, "y"), (2, low, "y"), (1, high, "x"))
        self.copies = [remote(place, mine.at[k].at[part], stage.at[i], send.at[4 + i], recv.at[4 + i], to) for i, (k, part, to) in enumerate(plan)]

    def pair(self, k):
        return remote(self.place, self.theirs.at[k % self.n_buf], self.got.at[k], self.send.at[k], self.recv.at[k], "c")

    def chip(self, k):
        self.pair(k).wait_recv()
        add_rows(self.mine.at[k], self.got.at[k], 0, 2 * self.h)

    def chip_x(self):
        self.chip(1)
        self.copies[0].start()

    def chip_y(self):
        self.chip(2)
        self.copies[1].start()

    def chip_d(self):
        self.chip(3)
        self.copies[2].start()
        self.copies[3].start()

    def turn(self):
        h = self.h
        self.copies[2].wait_recv()
        add_rows(self.mine.at[2], self.stage.at[2], 0, h)
        self.copies[4].start()
        self.copies[3].wait_recv()
        add_rows(self.mine.at[1], self.stage.at[3], h, h)
        self.copies[5].start()

    def near(self):
        h = self.h
        self.copies[0].wait_recv()
        add_rows(self.mine.at[0], self.stage.at[0], 0, h)
        self.copies[1].wait_recv()
        add_rows(self.mine.at[0], self.stage.at[1], h, h)

    def last(self):
        h = self.h
        self.copies[4].wait_recv()
        add_rows(self.mine.at[0], self.stage.at[4], 0, h)
        self.copies[5].wait_recv()
        add_rows(self.mine.at[0], self.stage.at[5], h, h)

    def drain(self, last):
        if last:
            for k in range(4 - self.n_buf, 4):
                self.pair(k).wait_send()
        for c in self.copies:
            c.wait_send()


def slot_ids(n_tok, cap):
    return lax.broadcasted_iota(jnp.int32, (n_tok, cap), 0).astype(F32)


def one_hot(tab, src, t, e, ids):
    return jnp.where(tab[src, t, 0, pl.ds(e, 1), :] == ids, 1.0, 0.0).astype(BF16)


def gated(tab, src, t, e, ids):
    return jnp.where(tab[src, t, 0, pl.ds(e, 1), :] == ids, tab[src, t, 1, pl.ds(e, 1), :], 0.0).astype(BF16)


def pick(weights, rows):
    return dot_ta(jnp.concatenate(weights, axis=1), rows).astype(BF16)


def experts_fwd(place, tab, t, k, z, w, os, mine, theirs, mid):
    n_exp, cap, n_tok = w[0].shape[0], tab.shape[4], z.shape[2]
    ids = slot_ids(n_tok, cap)
    src = [place.source(k, c) for c in range(2)]

    def step(i, _):
        mid(i)
        es = (2 * i, 2 * i + 1)
        x = [pick([one_hot(tab, src[c], t, e, ids) for e in es], z[k, c]) for c in range(2)]
        for j, e in enumerate(es):
            xe = jnp.concatenate([x[c][j * cap:(j + 1) * cap] for c in range(2)], axis=0)
            a = dot(xe, w[0][e])
            b = dot(xe, w[1][e])
            o = dot((a * jax.nn.sigmoid(a) * b).astype(BF16), w[2][e]).astype(BF16)
            rows = pl.ds(pl.multiple_of(e * cap, cap), cap)
            os[0, rows, :] = o[:cap]
            os[1, rows, :] = o[cap:]
        return 0
    lax.fori_loop(0, n_exp // 2, step, 0)
    mid(n_exp // 2)
    for c, p in ((1, theirs), (0, mine)):
        p[...] = dot(jnp.concatenate([gated(tab, src[c], t, e, ids) for e in range(n_exp)], axis=1), os[c])


def experts_bwd(place, tab, t, k, z, g, w, grads, os, mine, theirs, mid):
    n_exp, cap, n_tok = w[0].shape[0], tab.shape[4], z.shape[2]
    ids = slot_ids(n_tok, cap)
    src = [place.source(k, c) for c in range(2)]

    def step(i, _):
        mid(i)
        es = (2 * i, 2 * i + 1)
        x = [pick([one_hot(tab, src[c], t, e, ids) for e in es], z[k, c]) for c in range(2)]
        r = [pick([gated(tab, src[c], t, e, ids) for e in es], g[k, c]) for c in range(2)]
        for j, e in enumerate(es):
            xe = jnp.concatenate([x[c][j * cap:(j + 1) * cap] for c in range(2)], axis=0)
            re = jnp.concatenate([r[c][j * cap:(j + 1) * cap] for c in range(2)], axis=0)
            a = dot(xe, w[0][e])
            b = dot(xe, w[1][e])
            dm = dot_tb(re, w[2][e])
            sig = jax.nn.sigmoid(a)
            act = a * sig
            m = (act * b).astype(BF16)
            da = (dm * b * (sig * (1.0 + a * (1.0 - sig)))).astype(BF16)
            db = (dm * act).astype(BF16)
            o = (dot_tb(da, w[0][e]) + dot_tb(db, w[1][e])).astype(BF16)
            rows = pl.ds(pl.multiple_of(e * cap, cap), cap)
            os[0, rows, :] = o[:cap]
            os[1, rows, :] = o[cap:]
            grads[0][e] += dot_ta(xe, da)
            grads[1][e] += dot_ta(xe, db)
            grads[2][e] += dot_ta(m, re)
        return 0
    lax.fori_loop(0, n_exp // 2, step, 0)
    mid(n_exp // 2)
    for c, p in ((1, theirs), (0, mine)):
        p[...] = dot(jnp.concatenate([one_hot(tab, src[c], t, e, ids) for e in range(n_exp)], axis=1), os[c])


def add_hidden(h_ref, mixed):
    def step(i, _):
        rows = pl.ds(pl.multiple_of(i * ROWS, ROWS), ROWS)
        h_ref[rows, :] = (h_ref[rows, :].astype(F32) + mixed[rows, :]).astype(BF16)
        return 0
    lax.fori_loop(0, h_ref.shape[0] // ROWS, step, 0)


class Names:
    def __init__(self, names, refs):
        self.by = dict(zip(names, refs))

    def __call__(self, name):
        return self.by.get(name)


def moe_body(kinds, blocks, passes, names, *refs):
    ref = Names(names, refs)
    place = Place()
    load, store = ref("load"), ref("store")
    n_load, n_store = [0], [0]

    def fetch(a, b):
        n_load[0] += 1
        c = pltpu.make_async_copy(a, b, load.at[n_load[0] - 1])
        c.start()
        return c

    def put(a, b):
        n_store[0] += 1
        c = pltpu.make_async_copy(a, b, store.at[n_store[0] - 1])
        c.start()
        return c

    first_phase = ref("tab_out") is not None
    peers = [place.source(j // 2, j % 2) for j in range(1, 8)] if first_phase else list(place.near.values())
    greet(place, peers)

    w = [ref(n) for n in ("wg", "wu", "wd")]
    dense_w = [ref(n) for n in ("w1", "w2")]
    grads = [ref(n) for n in ("dg", "du", "dd")] if ref("dg") is not None else None
    tab, os = ref("tab"), ref("os")

    def fetch_experts(block):
        return [fetch(ref(n + "_in").at[0, block], v) for n, v in zip(("wg", "wu", "wd"), w)]

    def experts_of(block):
        return [pltpu.make_async_copy(ref(n + "_in").at[0, block], v, load.at[20 + i]) for i, (n, v) in enumerate(zip(("wg", "wu", "wd"), w))]

    def fetch_dense(block):
        return [fetch(ref(n + "_in").at[0, block], v) for n, v in zip(("w1", "w2"), dense_w)]

    def done(copies):
        for c in copies:
            c.wait()

    streams = []
    for s, kind in enumerate(kinds):
        st = dict(kind=kind, s=s, block=blocks[s], t=passes[s], z=ref(f"z{s}"), h=ref(f"h{s}"), x=ref(f"x{s}"), g=ref(f"g{s}"), rows=[])
        if kind != "first":
            st["rows"].append(Rows(place, st["z"], ref(f"z{s}_send"), ref(f"z{s}_recv")))
        else:
            st["rows"].append(Rows(place, st["g"], ref(f"g{s}_send"), ref(f"g{s}_recv")))
        st["sums"] = Sums(place, ref(f"mine{s}"), ref("theirs"), ref(f"got{s}"), ref(f"stage{s}"), ref(f"s{s}_send"), ref(f"s{s}_recv"))
        st["x_in"] = st["x"] if st["x"] is not None else st["z"].at[0, 0]
        streams.append(st)
    a, b = streams[0], streams[-1]
    two = len(streams) == 2
    back = next((st for st in streams if st["kind"] != "fwd"), None)
    order = [st for st in streams if st["kind"] != "first"]
    x_in = [[fetch(ref(f"x{st['s']}_in"), st["x_in"])] for st in streams]
    have = order[0]["block"]
    d_in = fetch_dense(have)
    e_in = fetch_experts(a["block"])
    later = []
    extra = None
    if back is not None and back["kind"] == "second":
        later.append(fetch(ref("g1_in"), back["g"]))
    if back is not None and back["kind"] == "first":
        later += [fetch(ref("g1_in"), back["g"].at[0, 0]), fetch(ref("z1_in"), back["z"]), fetch(ref("h1_in"), back["h"])] + x_in[1]
    if first_phase:
        extra = Rows(place, ref("more"), ref("more_send"), ref("more_recv"))
        later.append(fetch(ref("more_in"), ref("more").at[0, 0]))
    if first_phase:
        mail = ref("mail")
        me = place.source(0, 0)
        post = []

        def tables(name, base):
            slot_tables(ref("route_" + name), ref("gate_" + name), mail, base)
            part = pl.ds(base, 2)
            own.append(fetch(mail.at[me, part], tab.at[me, part]))
            for j, to in enumerate(peers):
                c = pltpu.make_async_remote_copy(src_ref=mail.at[to, part], dst_ref=tab.at[me, part], send_sem=ref("t_send").at[base // 2, j],
                                                 recv_sem=ref("t_recv").at[base // 2, j], device_id=(place.pp, to), device_id_type=MESH)
                c.start()
                post.append(c)
        own = []
    for st in order:
        done(x_in[st["s"]])
        if st["block"] != have:
            d_in = fetch_dense(st["block"])
            have = st["block"]
        done(d_in)
        d_in = []
        dense_fwd(st["x_in"], *dense_w, st["h"], st["z"].at[0, 0])
        if st is a:
            greeted(peers)
            st["rows"][0].start()
    end_dense = []
    if back is not None and have != back["block"]:
        end_dense = fetch_dense(back["block"])
    ends = []
    if first_phase:
        tables("bwd", 2)
        tables("fwd", 0)
        done(own)
    if grads is not None:
        for gr in grads:
            def clear(e, _, gr=gr):
                gr[e] = jnp.zeros(gr.shape[1:], F32)
                return 0
            lax.fori_loop(0, gr.shape[0], clear, 0)
    done(later)
    done(e_in)

    def unit(st, k, mid):
        sums = st["sums"]
        nb = sums.n_buf

        @pl.when(k >= nb)
        def _():
            sums.pair(k - nb).wait_send()
        if st is not a:
            @pl.when(k < nb)
            def _():
                a["sums"].pair(k + 4 - nb).wait_send()
        theirs = sums.theirs.at[k % nb]
        if st["kind"] == "fwd":
            experts_fwd(place, tab, st["t"], k, st["z"], w, os, sums.mine.at[k], theirs, mid)
        else:
            experts_bwd(place, tab, st["t"], k, st["z"], st["g"], w, grads, os, sums.mine.at[k], theirs, mid)
        sums.pair(k).start()

    def pass_xy(r):
        r.pass_x()
        r.pass_y()

    ra, rb, sa, sb = a["rows"][0], b["rows"][0], a["sums"], b["sums"]
    if two:
        before = {(0, 1): [lambda: pass_xy(ra), rb.start], (1, 0): [lambda: pass_xy(rb)], (1, 2): [rb.pass_d]}
        during = {(0, 2): [ra.pass_d, sa.chip_x], (0, 3): [sa.chip_y], (1, 0): [sa.chip_d], (1, 1): [lambda: sa.chip(0)],
                  (1, 2): [sa.turn, sb.chip_x], (1, 3): [sb.chip_y]}
    else:
        before = {(0, 0): [lambda: pass_xy(ra), extra.start] + [c.wait_recv for c in post[:7]]}
        during = {(0, 1): [ra.pass_d], (0, 2): [sa.chip_x], (0, 3): [sa.chip_y]}
    for s, st in enumerate(streams):
        at = 2 if st["kind"] == "fwd" else 1

        def loop(k, _, s=s, st=st, at=at):
            for kk in range(4):
                @pl.when(k == kk)
                def _(kk=kk):
                    for f in before.get((s, kk), []):
                        f()
                    st["rows"][0].ready(kk)

            def mid(i):
                if s == 0 and two:
                    @pl.when((k == 3) & (i == w[0].shape[0] // 2))
                    def _():
                        for c in experts_of(b["block"]):
                            c.start()
                for kk in range(4):
                    if (s, kk) in during:
                        @pl.when((k == kk) & (i == at))
                        def _(kk=kk):
                            for f in during[s, kk]:
                                f()
            unit(st, k, mid)
            return 0
        lax.fori_loop(0, 4, loop, 0)
        if s == 0 and two:
            done(experts_of(b["block"]))
        if st is back:
            ends += [put(gr, ref(n + "_out")) for gr, n in zip(grads, ("dg", "du", "dd"))]
    if first_phase:
        ends.append(put(a["z"], ref("z0_out")))
    sb.chip_d()
    if first_phase:
        pass_xy(extra)
    sb.chip(0)
    done(end_dense)
    if two:
        dense_slope(b["x"], dense_w[0], sb.got)
        sa.near()
        finish(a, ref, dense_w, put, ends, False)
    sb.turn()
    sb.near()
    if first_phase:
        extra.pass_d()
    if first_phase:
        for c in post[7:]:
            c.wait_recv()
        ends.append(put(tab, ref("tab_out")))
        for k in range(4):
            extra.ready(k)
        ends.append(put(ref("more"), ref("more_out")))
        extra.drain()
    finish(b, ref, dense_w, put, ends, True)
    if first_phase:
        for c in post:
            c.wait_send()
    for c in ends:
        c.wait()


def finish(st, ref, dense_w, put, ends, last):
    sums, s = st["sums"], st["s"]
    if st["kind"] == "fwd" and ref(f"h{s}_out") is not None:
        put(st["h"], ref(f"h{s}_out")).wait()
    sums.last()
    if st["kind"] == "fwd":
        add_hidden(st["h"], sums.mine.at[0])
        ends.append(put(st["h"], ref(f"y{s}_out")))
    else:
        dense_bwd(st["g"].at[0, 0], sums.mine.at[0], st["h"], st["x"], sums.got, *dense_w, st["x"])
        ends.append(put(st["x"], ref(f"y{s}_out")))
    sums.drain(last)
    st["rows"][0].drain()


def moe(kinds, blocks, passes, ins, out_names, weights, cid, n_buf):
    _, n, d = ins["x0_in"].shape
    ins = {nm: (v[0] if nm[0] == "x" else v) for nm, v in ins.items()}
    dma = pltpu.SemaphoreType.DMA
    ins.update(zip(("wg_in", "wu_in", "wd_in", "w1_in", "w2_in"), weights))
    shapes = [x.shape[2:] for x in weights]
    n_exp = shapes[0][0]
    groups = 8
    tab_shape = (groups, 4, 2, 8, 128)
    row = jax.ShapeDtypeStruct((n, d), BF16)
    every = jax.ShapeDtypeStruct((4, 2, n, d), BF16)
    made = {"tab_out": jax.ShapeDtypeStruct(tab_shape, F32), "z0_out": every, "more_out": every}
    made.update({nm + "_out": jax.ShapeDtypeStruct(sh, F32) for nm, sh in zip(("dg", "du", "dd"), shapes)})
    outs = {nm: made.get(nm, row) for nm in out_names}
    scratch = {nm: pltpu.VMEM(sh, BF16) for nm, sh in zip(("wg", "wu", "wd", "w1", "w2"), shapes)}
    scratch.update(os=pltpu.VMEM((2, n_exp * 128, d), BF16), theirs=pltpu.VMEM((n_buf, n, d), F32), load=dma((24,)), store=dma((12,)))
    slots = pltpu.VMEM((4, 2, n, d), BF16)
    if "tab_out" in outs:
        scratch.update(tab=pltpu.VMEM(tab_shape, F32), mail=pltpu.VMEM(tab_shape, F32), t_send=dma((2, 7)), t_recv=dma((2, 7)))
        scratch.update(more=slots, more_send=dma((N_AG,)), more_recv=dma((N_AG,)))
    for s, kind in enumerate(kinds):
        scratch.update({f"z{s}": slots, f"h{s}": pltpu.VMEM((n, d), BF16)})
        own = "g" if kind == "first" else "z"
        scratch.update({f"{own}{s}_send": dma((N_AG,)), f"{own}{s}_recv": dma((N_AG,))})
        if kind != "fwd":
            scratch.update({f"g{s}": slots, f"x{s}": pltpu.VMEM((n, d), BF16)})
            scratch.update({nm: pltpu.VMEM(sh, F32) for nm, sh in zip(("dg", "du", "dd"), shapes)})
        scratch.update({f"mine{s}": pltpu.VMEM((4, n, d), F32), f"got{s}": pltpu.VMEM((4, n, d), F32),
                        f"stage{s}": pltpu.VMEM((6, n // 2, d), F32), f"s{s}_send": dma((N_RS,)), f"s{s}_recv": dma((N_RS,))})
    small = ("tab", "route_fwd", "route_bwd", "gate_fwd", "gate_bwd")
    res = pl.pallas_call(
        functools.partial(moe_body, kinds, blocks, passes, list(ins) + list(outs) + list(scratch)), out_shape=list(outs.values()),
        in_specs=[VMEM if nm in small else ANY for nm in ins], out_specs=[ANY] * len(outs), scratch_shapes=list(scratch.values()),
        compiler_params=pltpu.CompilerParams(vmem_limit_bytes=67043328, collective_id=cid, has_side_effects=True),
        cost_estimate=cost(3e10, 5e7), name="moe_" + "_".join(kinds))(*ins.values())
    return dict(zip(outs, res))


def solution(mesh):
    stages = mesh.shape['pp']
    to_next = [(sender, (sender + 1) % stages) for sender in range(stages)]
    to_prev = [(sender, (sender - 1) % stages) for sender in range(stages)]

    def local_step(x_fwd, x_bwd, grad_in, dense_in, dense_out, exp_gate, exp_up, exp_down, route_fwd, gate_fwd, route_bwd, gate_bwd):
        weights = (exp_gate, exp_up, exp_down, dense_in, dense_out)
        turned = [jnp.swapaxes(v[0], 1, 2) for v in (route_fwd, route_bwd, gate_fwd, gate_bwd)]
        route = dict(zip(("route_fwd", "route_bwd", "gate_fwd", "gate_bwd"), turned))
        grads = ("dg_out", "du_out", "dd_out")
        one = moe(("fwd",), (0,), (2,), dict(route, x0_in=x_bwd, more_in=grad_in[0]), ("y0_out", "h0_out", "tab_out", "z0_out", "more_out"), weights, 0, 2)
        two = moe(("fwd", "second"), (0, 1), (0, 3), dict(tab=one["tab_out"], x0_in=x_fwd, x1_in=one["y0_out"][None], g1_in=one["more_out"]), ("y0_out", "y1_out") + grads, weights, 1, 2)
        three = moe(("fwd", "first"), (1, 0), (1, 2), dict(tab=one["tab_out"], x0_in=two["y0_out"][None], x1_in=x_bwd, h1_in=one["h0_out"], z1_in=one["z0_out"], g1_in=two["y1_out"]), ("y0_out", "y1_out") + grads, weights, 2, 2)
        y_next = lax.ppermute(three["y0_out"], 'pp', to_next)
        dx_prev = lax.ppermute(three["y1_out"], 'pp', to_prev)
        return (y_next[None], dx_prev[None]) + tuple(jnp.stack([three[g], two[g]])[None] for g in grads)

    tok_spec = P('pp', 'ep', None)
    dense_spec = P('pp', None, None, None)
    exp_spec = P('pp', None, 'ep', None, None)
    route_spec = P('pp', None, 'ep', None)
    return jax.shard_map(local_step, mesh=mesh, in_specs=(tok_spec, tok_spec, tok_spec, dense_spec, dense_spec, exp_spec, exp_spec, exp_spec, route_spec, route_spec, route_spec, route_spec), out_specs=(tok_spec, tok_spec, exp_spec, exp_spec, exp_spec), check_vma=False)
```

```python
import functools
from types import SimpleNamespace

import jax
import jax.numpy as jnp
from jax import lax
from jax.experimental import pallas as pl
from jax.experimental.pallas import tpu as pltpu
from jax.sharding import PartitionSpec as P

NORM_EPS = 1e-6
F32 = jnp.float32
BF16 = jnp.bfloat16
VMEM = pl.BlockSpec(memory_space=pltpu.VMEM)
ANY = pl.BlockSpec(memory_space=pl.ANY)


def dot(a, b):
    return lax.dot_general(a, b, (((1,), (0,)), ((), ())), preferred_element_type=F32)


def dot_ta(a, b):
    return lax.dot_general(a, b, (((0,), (0,)), ((), ())), preferred_element_type=F32)


def dot_tb(a, b):
    return lax.dot_general(a, b, (((1,), (1,)), ((), ())), preferred_element_type=F32)


def rms_norm(v):
    return v * lax.rsqrt(jnp.mean(v * v, axis=-1, keepdims=True) + NORM_EPS)


def rms_back(v, g):
    inv = lax.rsqrt(jnp.mean(v * v, axis=-1, keepdims=True) + NORM_EPS)
    proj = jnp.mean(g * v, axis=-1, keepdims=True)
    return inv * g - v * (inv * inv * inv) * proj


def cost(flops, nbytes):
    return pl.CostEstimate(flops=int(flops), bytes_accessed=int(nbytes), transcendentals=0)


ROWS = 256


def dense_fwd(x_ref, w1, w2, h_ref, z_ref):
    def step(i, _):
        rows = pl.ds(pl.multiple_of(i * ROWS, ROWS), ROWS)
        x = x_ref[rows, :].astype(F32)
        pre = dot(rms_norm(x).astype(BF16), w1[...])
        mid = (pre * jax.nn.sigmoid(pre)).astype(BF16)
        h = (x + dot(mid, w2[...])).astype(BF16)
        h_ref[rows, :] = h
        z_ref[rows, :] = rms_norm(h.astype(F32)).astype(BF16)
        return 0
    lax.fori_loop(0, x_ref.shape[0] // ROWS, step, 0)


def dense_slope(x_ref, w1, slope):
    half = slope.shape[2]

    def step(i, _):
        rows = pl.ds(pl.multiple_of(i * ROWS, ROWS), ROWS)
        pre = dot(rms_norm(x_ref[rows, :].astype(F32)).astype(BF16), w1[...])
        sig = jax.nn.sigmoid(pre)
        val = sig * (1.0 + pre * (1.0 - sig))
        slope[0, rows, :] = val[:, :half]
        slope[1, rows, :] = val[:, half:]
        return 0
    lax.fori_loop(0, x_ref.shape[0] // ROWS, step, 0)


def dense_bwd(g_ref, dz_ref, h_ref, x_ref, slope, w1, w2, o_ref, piece, size):
    def step(i, _):
        rows = pl.ds(pl.multiple_of(i * (x_ref.shape[0] // 2) + piece * size, size), size)
        x = x_ref[rows, :].astype(F32)
        dh = g_ref[rows, :].astype(F32) + rms_back(h_ref[rows, :].astype(F32), dz_ref[rows, :])
        turned = jnp.concatenate([slope[0, rows, :], slope[1, rows, :]], axis=1)
        dp = (dot_tb(dh.astype(BF16), w2[...]) * turned).astype(BF16)
        o_ref[rows, :] = (dh + rms_back(x, dot_tb(dp, w1[...]))).astype(BF16)
        return 0
    lax.fori_loop(0, 2, step, 0)


def slot_tables(route_ref, gate_ref, o_ref, base, t):
    _, top_k, n_tok = route_ref.shape
    groups = o_ref.shape[0]
    n_exp = groups * o_ref.shape[3]
    row = lax.broadcasted_iota(jnp.int32, (2 * n_exp, n_tok), 0)
    first = row < n_exp
    row_exp = jnp.where(first, row, row - n_exp)
    ids = lax.broadcasted_iota(jnp.int32, (2 * n_exp, n_tok), 1) + 1
    value = jnp.where(first, ids >> 4, ids & 15).astype(F32)
    slot = lax.broadcasted_iota(jnp.int32, (128, n_tok), 0)

    acc = jnp.zeros((3 * n_exp, 128), F32)
    for k in range(top_k):
        r = route_ref[t, k:k + 1, :]
        hit = (r >> 7) == row_exp
        left = jnp.concatenate([jnp.where(hit, value, 0.0), jnp.where(hit[:n_exp], gate_ref[t, k:k + 1, :].astype(F32), 0.0)], axis=0)
        right = jnp.where((r & 127) == slot, 1.0, 0.0).astype(BF16)
        acc += dot_tb(left.astype(BF16), right)
    tok = acc[:n_exp] * 16.0 + acc[n_exp:2 * n_exp] - 1.0
    gat = acc[2 * n_exp:]
    for g in range(groups):
        o_ref[g, base + t, 0] = tok[g * 8:(g + 1) * 8]
        o_ref[g, base + t, 1] = gat[g * 8:(g + 1) * 8]


MESH = pl.DeviceIdType.MESH
N_AG, N_RS, PIECES = 10, 14, 2


class Place:
    def __init__(self):
        me = lax.axis_index("ep")
        self.core, self.x, self.y = me % 2, (me // 2) % 2, me // 4
        self.pp = lax.axis_index("pp")
        self.near = {"c": me + 1 - 2 * self.core, "x": me + 2 - 4 * self.x, "y": me + 4 - 8 * self.y}

    def source(self, k, c):
        x, y = (self.x + k % 2) % 2, (self.y + k // 2) % 2
        core = self.core if c == 0 else 1 - self.core
        return y * 4 + x * 2 + core


def remote(place, src, dst, send, recv, to):
    return pltpu.make_async_remote_copy(src_ref=src, dst_ref=dst, send_sem=send, recv_sem=recv, device_id=(place.pp, place.near[to]), device_id_type=MESH)


def greet(place, peers):
    for peer in peers:
        pl.semaphore_signal(pltpu.get_barrier_semaphore(), inc=1, device_id=(place.pp, peer), device_id_type=MESH)


def greeted(peers):
    pl.semaphore_wait(pltpu.get_barrier_semaphore(), len(peers))


class Rows:
    def __init__(self, place, slots, send, recv, split=False):
        h = slots.shape[2] // 2
        self.split = split
        plan = ((0, 0, 1, 0, "x", None), (0, 0, 2, 0, "y", None), (0, 0, 0, 1, "c", None), (1, 0, 3, 0, "y", (0, h)), (1, 0, 1, 1, "c", None),
                (2, 0, 3, 0, "x", (h, h)), (2, 0, 2, 1, "c", None), (3, 0, 3, 1, "c", None))
        if split:
            q = h // 2
            plan = ((0, 0, 1, 0, "x", (0, q)), (0, 0, 2, 0, "y", (0, q))) + plan[2:] + ((0, 0, 1, 0, "x", (q, 3 * q)), (0, 0, 2, 0, "y", (q, 3 * q)))
        self.copies = []
        for i, (ks, cs, kd, cd, to, part) in enumerate(plan):
            s, d = slots.at[ks, cs], slots.at[kd, cd]
            if part is not None:
                s, d = s.at[pl.ds(*part)], d.at[pl.ds(*part)]
            self.copies.append(remote(place, s, d, send.at[i], recv.at[i], to))

    def start(self):
        for i in (0, 1, 2):
            self.copies[i].start()

    def rest(self):
        self.copies[8].start()
        self.copies[9].start()

    def pass_x(self):
        self.copies[0].wait_recv()
        if self.split:
            self.copies[8].wait_recv()
        self.copies[3].start()
        self.copies[4].start()

    def pass_y(self):
        self.copies[1].wait_recv()
        if self.split:
            self.copies[9].wait_recv()
        self.copies[5].start()
        self.copies[6].start()

    def pass_d(self):
        self.copies[3].wait_recv()
        self.copies[5].wait_recv()
        self.copies[7].start()

    def ready(self, k):
        self.copies[(2, 4, 6, 7)[k]].wait_recv()

    def drain(self):
        for c in self.copies:
            c.wait_send()


def add_rows(dst, b, lo, n):
    def step(i, _):
        at = pl.multiple_of(i * 64, 64)
        rows = pl.ds(lo + at, 64)
        dst[rows, :] = dst[rows, :] + b[pl.ds(at, 64), :]
        return 0
    lax.fori_loop(0, n // 64, step, 0)


class Sums:
    def __init__(self, place, mine, theirs, got, stage, send, recv):
        h = mine.shape[1] // 2
        self.h, self.q, self.mine, self.got, self.stage, self.recv, self.send = h, h // PIECES, mine, got, stage, recv, send
        self.theirs, self.n_buf, self.place = theirs, theirs.shape[0], place

        def move(sem, slot, k, at, low, n, to):
            return remote(place, mine.at[k].at[pl.ds(at + low, n)], stage.at[slot].at[pl.ds(low, n)], send.at[sem], recv.at[sem], to)
        self.near_x, self.near_y = move(4, 0, 1, 0, 0, h, "x"), move(5, 1, 2, h, 0, h, "y")
        q = self.q
        self.far_y = [move(6 + p, 2, 3, 0, p * q, q, "x") for p in range(PIECES)]
        self.far_x = [move(8 + p, 3, 3, h, p * q, q, "y") for p in range(PIECES)]
        self.last_y = [move(10 + p, 4, 2, 0, p * q, q, "y") for p in range(PIECES)]
        self.last_x = [move(12 + p, 5, 1, h, p * q, q, "x") for p in range(PIECES)]

    def pair(self, k):
        return remote(self.place, self.theirs.at[k % self.n_buf], self.got.at[k], self.send.at[k], self.recv.at[k], "c")

    def add(self, k, lo, slot, low, n):
        add_rows(self.mine.at[k], self.stage.at[slot].at[pl.ds(low, n)], lo + low, n)

    def chip(self, k):
        self.pair(k).wait_recv()
        add_rows(self.mine.at[k], self.got.at[k], 0, 2 * self.h)

    def chip_x(self):
        self.chip(1)
        self.near_x.start()

    def chip_y(self):
        self.chip(2)
        self.near_y.start()

    def chip_d(self):
        self.chip(3)
        for p in range(PIECES):
            self.far_y[p].start()
            self.far_x[p].start()

    def turn(self):
        for p in range(PIECES):
            self.far_y[p].wait_recv()
            self.add(2, 0, 2, p * self.q, self.q)
            self.last_y[p].start()
            self.far_x[p].wait_recv()
            self.add(1, self.h, 3, p * self.q, self.q)
            self.last_x[p].start()

    def near(self):
        self.near_x.wait_recv()
        self.add(0, 0, 0, 0, self.h)
        self.near_y.wait_recv()
        self.add(0, self.h, 1, 0, self.h)

    def last(self, p):
        self.last_y[p].wait_recv()
        self.add(0, 0, 4, p * self.q, self.q)
        self.last_x[p].wait_recv()
        self.add(0, self.h, 5, p * self.q, self.q)

    def drain(self, last):
        if last:
            for k in range(4 - self.n_buf, 4):
                self.pair(k).wait_send()
        for c in [self.near_x, self.near_y] + self.far_x + self.far_y + self.last_x + self.last_y:
            c.wait_send()


def slot_ids(n_tok, cap):
    return lax.broadcasted_iota(jnp.int32, (n_tok, cap), 0).astype(F32)


def one_hot(tab, src, t, e, ids):
    return jnp.where(tab[src, t, 0, pl.ds(e, 1), :] == ids, 1.0, 0.0).astype(BF16)


def gated(tab, src, t, e, ids):
    return jnp.where(tab[src, t, 0, pl.ds(e, 1), :] == ids, tab[src, t, 1, pl.ds(e, 1), :], 0.0).astype(BF16)


def pick(weights, rows):
    return dot_ta(jnp.concatenate(weights, axis=1), rows).astype(BF16)


def experts_fwd(place, tab, t, k, z, w, os, mine, theirs, mid):
    n_exp, cap, n_tok = w[0].shape[0], tab.shape[4], z.shape[2]
    ids = slot_ids(n_tok, cap)
    src = [place.source(k, c) for c in range(2)]

    def step(i, _):
        mid(i)
        es = (2 * i, 2 * i + 1)
        x = [pick([one_hot(tab, src[c], t, e, ids) for e in es], z[k, c]) for c in range(2)]
        for j, e in enumerate(es):
            xe = jnp.concatenate([x[c][j * cap:(j + 1) * cap] for c in range(2)], axis=0)
            a = dot(xe, w[0][e])
            b = dot(xe, w[1][e])
            o = dot((a * jax.nn.sigmoid(a) * b).astype(BF16), w[2][e]).astype(BF16)
            rows = pl.ds(pl.multiple_of(e * cap, cap), cap)
            os[0, rows, :] = o[:cap]
            os[1, rows, :] = o[cap:]
        return 0
    lax.fori_loop(0, n_exp // 2, step, 0)
    mid(n_exp // 2)
    for c, p in ((1, theirs), (0, mine)):
        p[...] = dot(jnp.concatenate([gated(tab, src[c], t, e, ids) for e in range(n_exp)], axis=1), os[c])


def experts_bwd(place, tab, t, k, z, g, w, grads, os, mine, theirs, mid):
    n_exp, cap, n_tok = w[0].shape[0], tab.shape[4], z.shape[2]
    ids = slot_ids(n_tok, cap)
    src = [place.source(k, c) for c in range(2)]

    def step(i, _):
        mid(i)
        es = (2 * i, 2 * i + 1)
        x = [pick([one_hot(tab, src[c], t, e, ids) for e in es], z[k, c]) for c in range(2)]
        r = [pick([gated(tab, src[c], t, e, ids) for e in es], g[k, c]) for c in range(2)]
        for j, e in enumerate(es):
            xe = jnp.concatenate([x[c][j * cap:(j + 1) * cap] for c in range(2)], axis=0)
            re = jnp.concatenate([r[c][j * cap:(j + 1) * cap] for c in range(2)], axis=0)
            a = dot(xe, w[0][e])
            b = dot(xe, w[1][e])
            dm = dot_tb(re, w[2][e])
            sig = jax.nn.sigmoid(a)
            act = a * sig
            m = (act * b).astype(BF16)
            da = (dm * b * (sig * (1.0 + a * (1.0 - sig)))).astype(BF16)
            db = (dm * act).astype(BF16)
            o = (dot_tb(da, w[0][e]) + dot_tb(db, w[1][e])).astype(BF16)
            rows = pl.ds(pl.multiple_of(e * cap, cap), cap)
            os[0, rows, :] = o[:cap]
            os[1, rows, :] = o[cap:]
            grads[0][e] += dot_ta(xe, da)
            grads[1][e] += dot_ta(xe, db)
            grads[2][e] += dot_ta(m, re)
        return 0
    lax.fori_loop(0, n_exp // 2, step, 0)
    mid(n_exp // 2)
    for c, p in ((1, theirs), (0, mine)):
        p[...] = dot(jnp.concatenate([one_hot(tab, src[c], t, e, ids) for e in range(n_exp)], axis=1), os[c])


def add_hidden(h_ref, mixed):
    def step(i, _):
        rows = pl.ds(pl.multiple_of(i * ROWS, ROWS), ROWS)
        h_ref[rows, :] = (h_ref[rows, :].astype(F32) + mixed[rows, :]).astype(BF16)
        return 0
    lax.fori_loop(0, h_ref.shape[0] // ROWS, step, 0)


def spaces(tree):
    if isinstance(tree, dict):
        return SimpleNamespace(**{k: spaces(v) for k, v in tree.items()})
    return tuple(spaces(v) for v in tree) if isinstance(tree, tuple) else tree


class Local:
    def __init__(self, sems):
        self.sems, self.used = sems, 0

    def make(self, a, b):
        self.used += 1
        return pltpu.make_async_copy(a, b, self.sems.at[self.used - 1])

    def __call__(self, a, b):
        c = self.make(a, b)
        c.start()
        return c


def done(copies):
    for c in copies:
        c.wait()


FWD, SECOND, FIRST = range(3)


def moe_body(kinds, blocks, passes, trees, *refs):
    arg, out, own = (spaces(v) for v in jax.tree.unflatten(trees, refs))
    place = Place()
    fetch, put = Local(own.load), Local(own.store)
    start = kinds == (FWD,)
    peers = [place.source(j // 2, j % 2) for j in range(1, 8)] if start else list(place.near.values())
    ships = kinds[-1] == FIRST
    n_stage = lax.axis_size("pp")
    nxt, prv = lax.rem(place.pp + 1, n_stage), lax.rem(place.pp + n_stage - 1, n_stage)
    greet(place, peers)
    if ships:
        for stage in (nxt, prv):
            pl.semaphore_signal(pltpu.get_barrier_semaphore(), inc=1, device_id=(stage, place.source(0, 0)), device_id_type=MESH)

    def fetch_experts(block, make=fetch):
        return [make(a.at[0, block], v) for a, v in zip(arg.experts, own.experts)]

    def fetch_dense(block):
        return [fetch(a.at[0, block], v) for a, v in zip(arg.dense, own.dense)]

    streams = []
    for s, kind in enumerate(kinds):
        o = own.streams[s]
        st = SimpleNamespace(kind=kind, block=blocks[s], t=passes[s], arg=arg.streams[s], out=out.streams[s], z=o.z, h=o.h, x=o.x, g=o.g)
        st.rows = Rows(place, o.g if kind == FIRST else o.z, o.row_send, o.row_recv)
        st.sums = Sums(place, o.mine, own.theirs, o.got, o.stage, o.sum_send, o.sum_recv)
        st.x_in = o.z.at[0, 0] if o.x is None else o.x
        streams.append(st)
    a, b = streams[0], streams[-1]
    two = len(streams) == 2
    tab = own.tab
    later, ends, post = [], [], []
    extra = None
    if start:
        extra = Rows(place, own.more, own.more_send, own.more_recv, True)
        more_in = fetch(arg.more, own.more.at[0, 0])
        later += [fetch(r, v) for r, v in zip(arg.routes, own.routes)]
    x_in = [[fetch(st.arg.x, st.x_in)] for st in streams]
    have = a.block
    d_in = fetch_dense(have)
    e_in = fetch_experts(a.block)
    if not start:
        later.append(fetch(arg.tab, tab))
        if b.kind == SECOND:
            later.append(fetch(b.arg.g, b.g))
        else:
            later += [fetch(b.arg.g, b.g.at[0, 0]), fetch(b.arg.z, b.z), fetch(b.arg.h, b.h)] + x_in[1]

    def tables(t):
        routes = own.routes[2 * (t // 2):2 * (t // 2) + 2]
        slot_tables(*routes, own.mail, t - t % 2, t % 2)
        me = place.source(0, 0)
        later.append(fetch(own.mail.at[me, t], tab.at[me, t]))
        for j, to in enumerate(peers):
            c = pltpu.make_async_remote_copy(src_ref=own.mail.at[to, t], dst_ref=tab.at[me, t], send_sem=own.tab_send.at[t, j],
                                             recv_sem=own.tab_recv.at[t, j], device_id=(place.pp, to), device_id_type=MESH)
            c.start()
            post.append(c)

    if start:
        greeted(peers)
        more_in.wait()
        extra.start()
        done(later)
        later = []
        tables(2)
    for st in streams:
        if st.kind == FIRST:
            continue
        done(x_in[0 if st is a else 1])
        if st.block != have:
            d_in = fetch_dense(st.block)
            have = st.block
        done(d_in)
        d_in = []
        dense_fwd(st.x_in, *own.dense, st.h, st.z.at[0, 0])
        if st is a:
            if not start:
                greeted(peers + [nxt, prv] if ships else peers)
            st.rows.start()
    end_dense = fetch_dense(b.block) if have != b.block else []
    if start:
        for t in (3, 0, 1):
            tables(t)
    if b.kind != FWD:
        for gr in own.grads:
            def clear(e, _, gr=gr):
                gr[e] = jnp.zeros(gr.shape[1:], F32)
                return 0
            lax.fori_loop(0, gr.shape[0], clear, 0)
    done(later)
    done(e_in)
    swap = fetch_experts(b.block, fetch.make) if two else []

    def unit(st, k, mid):
        sums = st.sums
        nb = sums.n_buf

        @pl.when(k >= nb)
        def _():
            sums.pair(k - nb).wait_send()
        if st is not a:
            @pl.when(k < nb)
            def _():
                a.sums.pair(k + 4 - nb).wait_send()
        theirs = sums.theirs.at[k % nb]
        if st.kind == FWD:
            experts_fwd(place, tab, st.t, k, st.z, own.experts, own.os, sums.mine.at[k], theirs, mid)
        else:
            experts_bwd(place, tab, st.t, k, st.z, st.g, own.experts, own.grads, own.os, sums.mine.at[k], theirs, mid)
        sums.pair(k).start()

    def pass_xy(r):
        r.pass_x()
        r.pass_y()

    ra, rb, sa, sb = a.rows, b.rows, a.sums, b.sums
    if two:
        before = {(0, 1): [lambda: pass_xy(ra), rb.start], (1, 0): [lambda: pass_xy(rb)], (1, 2): [rb.pass_d]}
        during = {(0, 2): [ra.pass_d, sa.chip_x], (0, 3): [sa.chip_y], (1, 0): [sa.chip_d], (1, 1): [lambda: sa.chip(0)],
                  (1, 2): [sa.turn, sb.chip_x], (1, 3): [sb.chip_y]}
    else:
        before = {(0, 0): [c.wait_recv for c in post[:7]], (0, 1): [lambda: pass_xy(ra), extra.rest]}
        during = {(0, 2): [ra.pass_d, sa.chip_x], (0, 3): [sa.chip_y]}
    n_step = own.experts[0].shape[0] // 2
    for s, st in enumerate(streams):
        at = 2 if st.kind == FWD else 1

        def loop(k, _, s=s, st=st, at=at):
            for kk in range(4):
                @pl.when(k == kk)
                def _(kk=kk):
                    for f in before.get((s, kk), []):
                        f()
                    st.rows.ready(kk)

            def mid(i):
                if s == 0 and two:
                    @pl.when((k == 3) & (i == n_step))
                    def _():
                        for c in swap:
                            c.start()
                for kk in range(4):
                    if (s, kk) in during:
                        @pl.when((k == kk) & (i == at))
                        def _(kk=kk):
                            for f in during[s, kk]:
                                f()
            unit(st, k, mid)
            return 0
        lax.fori_loop(0, 4, loop, 0)
        if s == 0:
            done(swap)
    if b.kind != FWD:
        ends += [put(gr, o) for gr, o in zip(own.grads, out.grads)]
    sb.chip_d()
    if start:
        ends.append(put(a.z, out.z))
        pass_xy(extra)
    sb.chip(0)
    done(end_dense)
    if two:
        dense_slope(b.x, own.dense[0], sb.got)
        sa.near()
        ship = None
        if ships:
            ship = pltpu.make_async_remote_copy(src_ref=a.h, dst_ref=a.out.y, send_sem=own.ship.at[0], recv_sem=own.ship.at[1],
                                                device_id=(nxt, place.source(0, 0)), device_id_type=MESH)
        finish(a, own.dense, put, ends, False, ship)
    elif a.out.h is not None:
        put(a.h, a.out.h).wait()
    sb.near()
    sb.turn()
    if start:
        extra.pass_d()
        for c in post[7:]:
            c.wait_recv()
        ends.append(put(tab, out.tab))
        for k in range(4):
            extra.ready(k)
        ends.append(put(own.more, out.more))
        extra.drain()
    finish(b, own.dense, put, ends, True)
    for c in post:
        c.wait_send()
    done(ends)


def finish(st, dense, put, ends, last, ship=None):
    sums = st.sums
    for p in range(PIECES):
        sums.last(p)
        if st.kind != FWD:
            dense_bwd(st.g.at[0, 0], sums.mine.at[0], st.h, st.x, sums.got, *dense, st.x, p, sums.q)
            for low in (0, sums.h):
                rows = pl.ds(low + p * sums.q, sums.q)
                ends.append(put(st.x.at[rows], st.out.y.at[rows]))
    if st.kind == FWD:
        add_hidden(st.h, sums.mine.at[0])
        if ship is None:
            ends.append(put(st.h, st.out.y))
        else:
            ship.start()
            ends.append(ship)
    sums.drain(last)
    st.rows.drain()


def moe(kinds, blocks, passes, args, weights, cid, n_buf=2):
    n, d = args["streams"][0]["x"].shape
    experts, dense = weights[:3], weights[3:]
    start = kinds == (FWD,)
    dma, vmem = pltpu.SemaphoreType.DMA, pltpu.VMEM
    shapes = [v.shape[2:] for v in experts]
    n_exp = shapes[0][0]
    tab = (8, 4, 2, 8, 128)
    every = (4, 2, n, d)
    slots = vmem(every, BF16)
    give = jax.ShapeDtypeStruct
    args = dict(args, experts=tuple(experts), dense=tuple(dense))
    outs = dict(streams=tuple(dict(y=give((n, d), BF16), h=give((n, d), BF16) if start else None) for _ in kinds))
    own = dict(experts=tuple(vmem(v, BF16) for v in shapes), dense=tuple(vmem(v.shape[2:], BF16) for v in dense), os=vmem((2, n_exp * 128, d), BF16),
               theirs=vmem((n_buf, n, d), F32), load=dma((24,)), store=dma((16,)), ship=dma((2,)), tab=vmem(tab, F32))
    if start:
        outs.update(tab=give(tab, F32), z=give(every, BF16), more=give(every, BF16))
        own.update(mail=vmem(tab, F32), tab_send=dma((4, 7)), tab_recv=dma((4, 7)), more=slots, more_send=dma((N_AG,)), more_recv=dma((N_AG,)),
                   routes=tuple(vmem(v.shape, v.dtype) for v in args["routes"]))
    else:
        outs.update(grads=tuple(give(v, F32) for v in shapes))
        own.update(grads=tuple(vmem(v, F32) for v in shapes))
    own.update(streams=tuple(dict(
        z=slots, h=vmem((n, d), BF16), x=vmem((n, d), BF16) if kind != FWD else None, g=slots if kind != FWD else None, row_send=dma((N_AG,)), row_recv=dma((N_AG,)),
        mine=vmem((4, n, d), F32), got=vmem((4, n, d), F32), stage=vmem((6, n // 2, d), F32), sum_send=dma((N_RS,)), sum_recv=dma((N_RS,))) for kind in kinds))
    flat_in, _ = jax.tree.flatten(args)
    flat_out, out_tree = jax.tree.flatten(outs)
    flat_own, _ = jax.tree.flatten(own)
    _, trees = jax.tree.flatten((args, outs, own))
    res = pl.pallas_call(
        functools.partial(moe_body, kinds, blocks, passes, trees), out_shape=flat_out, in_specs=[ANY] * len(flat_in), out_specs=[ANY] * len(flat_out),
        scratch_shapes=flat_own, compiler_params=pltpu.CompilerParams(vmem_limit_bytes=67043328, collective_id=cid, has_side_effects=True),
        cost_estimate=cost(3e10, 5e7), name=f"moe_{cid}")(*flat_in)
    return spaces(jax.tree.unflatten(out_tree, res))


def solution(mesh):
    stages = mesh.shape['pp']
    to_prev = [(sender, (sender - 1) % stages) for sender in range(stages)]

    def local_step(x_fwd, x_bwd, grad_in, dense_in, dense_out, exp_gate, exp_up, exp_down, route_fwd, gate_fwd, route_bwd, gate_bwd):
        weights = (exp_gate, exp_up, exp_down, dense_in, dense_out)
        routes = tuple(jnp.swapaxes(v[0], 1, 2) for v in (route_fwd, gate_fwd, route_bwd, gate_bwd))
        one = moe((FWD,), (0,), (2,), dict(routes=routes, more=grad_in[0], streams=(dict(x=x_bwd[0]),)), weights, 0)
        mid = one.streams[0]
        two = moe((FWD, SECOND), (0, 1), (0, 3), dict(tab=one.tab, streams=(dict(x=x_fwd[0]), dict(x=mid.y, g=one.more))), weights, 1)
        back = dict(x=x_bwd[0], h=mid.h, z=one.z, g=two.streams[1].y)
        three = moe((FWD, FIRST), (1, 0), (1, 2), dict(tab=one.tab, streams=(dict(x=two.streams[0].y), back)), weights, 2)
        dx_prev = lax.ppermute(three.streams[1].y, 'pp', to_prev)
        return (three.streams[0].y[None], dx_prev[None]) + tuple(jnp.stack([p, q])[None] for p, q in zip(three.grads, two.grads))

    tok_spec = P('pp', 'ep', None)
    dense_spec = P('pp', None, None, None)
    exp_spec = P('pp', None, 'ep', None, None)
    route_spec = P('pp', None, 'ep', None)
    return jax.shard_map(local_step, mesh=mesh, in_specs=(tok_spec, tok_spec, tok_spec, dense_spec, dense_spec, exp_spec, exp_spec, exp_spec, route_spec, route_spec, route_spec, route_spec), out_specs=(tok_spec, tok_spec, exp_spec, exp_spec, exp_spec), check_vma=False)
```

```python
import functools
from types import SimpleNamespace

import jax
import jax.numpy as jnp
from jax import lax
from jax.experimental import pallas as pl
from jax.experimental.pallas import tpu as pltpu
from jax.sharding import PartitionSpec as P

NORM_EPS = 1e-6
F32 = jnp.float32
BF16 = jnp.bfloat16
VMEM = pl.BlockSpec(memory_space=pltpu.VMEM)
ANY = pl.BlockSpec(memory_space=pl.ANY)


def dot(a, b):
    return lax.dot_general(a, b, (((1,), (0,)), ((), ())), preferred_element_type=F32)


def dot_ta(a, b):
    return lax.dot_general(a, b, (((0,), (0,)), ((), ())), preferred_element_type=F32)


def dot_tb(a, b):
    return lax.dot_general(a, b, (((1,), (1,)), ((), ())), preferred_element_type=F32)


def rms_norm(v):
    return v * lax.rsqrt(jnp.mean(v * v, axis=-1, keepdims=True) + NORM_EPS)


def rms_back(v, g):
    inv = lax.rsqrt(jnp.mean(v * v, axis=-1, keepdims=True) + NORM_EPS)
    proj = jnp.mean(g * v, axis=-1, keepdims=True)
    return inv * g - v * (inv * inv * inv) * proj


def cost(flops, nbytes):
    return pl.CostEstimate(flops=int(flops), bytes_accessed=int(nbytes), transcendentals=0)


ROWS = 256


def dense_fwd(x_ref, w1, w2, h_ref, z_ref):
    def step(i, _):
        rows = pl.ds(pl.multiple_of(i * ROWS, ROWS), ROWS)
        x = x_ref[rows, :].astype(F32)
        pre = dot(rms_norm(x).astype(BF16), w1[...])
        mid = (pre * jax.nn.sigmoid(pre)).astype(BF16)
        h = (x + dot(mid, w2[...])).astype(BF16)
        h_ref[rows, :] = h
        z_ref[rows, :] = rms_norm(h.astype(F32)).astype(BF16)
        return 0
    lax.fori_loop(0, x_ref.shape[0] // ROWS, step, 0)


def dense_slope(x_ref, w1, slope):
    half = slope.shape[2]

    def step(i, _):
        rows = pl.ds(pl.multiple_of(i * ROWS, ROWS), ROWS)
        pre = dot(rms_norm(x_ref[rows, :].astype(F32)).astype(BF16), w1[...])
        sig = jax.nn.sigmoid(pre)
        val = sig * (1.0 + pre * (1.0 - sig))
        slope[0, rows, :] = val[:, :half]
        slope[1, rows, :] = val[:, half:]
        return 0
    lax.fori_loop(0, x_ref.shape[0] // ROWS, step, 0)


def dense_bwd(g_ref, dz_ref, h_ref, x_ref, slope, w1, w2, o_ref, piece, size):
    def step(i, _):
        rows = pl.ds(pl.multiple_of(i * (x_ref.shape[0] // 2) + piece * size, size), size)
        x = x_ref[rows, :].astype(F32)
        dh = g_ref[rows, :].astype(F32) + rms_back(h_ref[rows, :].astype(F32), dz_ref[rows, :])
        turned = jnp.concatenate([slope[0, rows, :], slope[1, rows, :]], axis=1)
        dp = (dot_tb(dh.astype(BF16), w2[...]) * turned).astype(BF16)
        o_ref[rows, :] = (dh + rms_back(x, dot_tb(dp, w1[...]))).astype(BF16)
        return 0
    lax.fori_loop(0, 2, step, 0)


def slot_tables(route_ref, gate_ref, o_ref, base, t):
    _, top_k, n_tok = route_ref.shape
    groups = o_ref.shape[0]
    n_exp = groups * o_ref.shape[3]
    row = lax.broadcasted_iota(jnp.int32, (2 * n_exp, n_tok), 0)
    first = row < n_exp
    row_exp = jnp.where(first, row, row - n_exp)
    ids = lax.broadcasted_iota(jnp.int32, (2 * n_exp, n_tok), 1) + 1
    value = jnp.where(first, ids >> 4, ids & 15).astype(F32)
    slot = lax.broadcasted_iota(jnp.int32, (128, n_tok), 0)

    acc = jnp.zeros((3 * n_exp, 128), F32)
    for k in range(top_k):
        r = route_ref[t, k:k + 1, :]
        hit = (r >> 7) == row_exp
        left = jnp.concatenate([jnp.where(hit, value, 0.0), jnp.where(hit[:n_exp], gate_ref[t, k:k + 1, :].astype(F32), 0.0)], axis=0)
        right = jnp.where((r & 127) == slot, 1.0, 0.0).astype(BF16)
        acc += dot_tb(left.astype(BF16), right)
    tok = acc[:n_exp] * 16.0 + acc[n_exp:2 * n_exp] - 1.0
    gat = acc[2 * n_exp:]
    for g in range(groups):
        o_ref[g, base + t, 0] = tok[g * 8:(g + 1) * 8]
        o_ref[g, base + t, 1] = gat[g * 8:(g + 1) * 8]


MESH = pl.DeviceIdType.MESH
N_AG, N_RS, PIECES = 10, 22, 4


class Place:
    def __init__(self):
        me = lax.axis_index("ep")
        self.core, self.x, self.y = me % 2, (me // 2) % 2, me // 4
        self.pp = lax.axis_index("pp")
        self.near = {"c": me + 1 - 2 * self.core, "x": me + 2 - 4 * self.x, "y": me + 4 - 8 * self.y}

    def source(self, k, c):
        x, y = (self.x + k % 2) % 2, (self.y + k // 2) % 2
        core = self.core if c == 0 else 1 - self.core
        return y * 4 + x * 2 + core


def remote(place, src, dst, send, recv, to):
    return pltpu.make_async_remote_copy(src_ref=src, dst_ref=dst, send_sem=send, recv_sem=recv, device_id=(place.pp, place.near[to]), device_id_type=MESH)


def greet(place, peers):
    for peer in peers:
        pl.semaphore_signal(pltpu.get_barrier_semaphore(), inc=1, device_id=(place.pp, peer), device_id_type=MESH)


def greeted(peers):
    pl.semaphore_wait(pltpu.get_barrier_semaphore(), len(peers))


class Rows:
    def __init__(self, place, slots, send, recv, split=False):
        h = slots.shape[2] // 2
        self.split = split
        plan = ((0, 0, 1, 0, "x", None), (0, 0, 2, 0, "y", None), (0, 0, 0, 1, "c", None), (1, 0, 3, 0, "y", (0, h)), (1, 0, 1, 1, "c", None),
                (2, 0, 3, 0, "x", (h, h)), (2, 0, 2, 1, "c", None), (3, 0, 3, 1, "c", None))
        if split:
            q = h // 2
            plan = ((0, 0, 1, 0, "x", (0, q)), (0, 0, 2, 0, "y", (0, q))) + plan[2:] + ((0, 0, 1, 0, "x", (q, 3 * q)), (0, 0, 2, 0, "y", (q, 3 * q)))
        self.copies = []
        for i, (ks, cs, kd, cd, to, part) in enumerate(plan):
            s, d = slots.at[ks, cs], slots.at[kd, cd]
            if part is not None:
                s, d = s.at[pl.ds(*part)], d.at[pl.ds(*part)]
            self.copies.append(remote(place, s, d, send.at[i], recv.at[i], to))

    def start(self):
        for i in (0, 1, 2):
            self.copies[i].start()

    def rest(self):
        self.copies[8].start()
        self.copies[9].start()

    def pass_x(self):
        self.copies[0].wait_recv()
        if self.split:
            self.copies[8].wait_recv()
        self.copies[3].start()
        self.copies[4].start()

    def pass_y(self):
        self.copies[1].wait_recv()
        if self.split:
            self.copies[9].wait_recv()
        self.copies[5].start()
        self.copies[6].start()

    def pass_d(self):
        self.copies[3].wait_recv()
        self.copies[5].wait_recv()
        self.copies[7].start()

    def ready(self, k):
        self.copies[(2, 4, 6, 7)[k]].wait_recv()

    def drain(self):
        for c in self.copies:
            c.wait_send()


def add_rows(dst, b, lo, n):
    def step(i, _):
        at = pl.multiple_of(i * 64, 64)
        rows = pl.ds(lo + at, 64)
        dst[rows, :] = dst[rows, :] + b[pl.ds(at, 64), :]
        return 0
    lax.fori_loop(0, n // 64, step, 0)


class Sums:
    def __init__(self, place, mine, theirs, got, stage, send, recv):
        h = mine.shape[1] // 2
        self.h, self.q, self.mine, self.got, self.stage, self.recv, self.send = h, h // PIECES, mine, got, stage, recv, send
        self.theirs, self.n_buf, self.place = theirs, theirs.shape[0], place

        def move(sem, slot, k, at, low, n, to):
            return remote(place, mine.at[k].at[pl.ds(at + low, n)], stage.at[slot].at[pl.ds(low, n)], send.at[sem], recv.at[sem], to)
        self.near_x, self.near_y = move(4, 0, 1, 0, 0, h, "x"), move(5, 1, 2, h, 0, h, "y")
        q = self.q
        self.far_y = [move(6 + 0 * PIECES + p, 2, 3, 0, p * q, q, "x") for p in range(PIECES)]
        self.far_x = [move(6 + 1 * PIECES + p, 3, 3, h, p * q, q, "y") for p in range(PIECES)]
        self.last_y = [move(6 + 2 * PIECES + p, 4, 2, 0, p * q, q, "y") for p in range(PIECES)]
        self.last_x = [move(6 + 3 * PIECES + p, 5, 1, h, p * q, q, "x") for p in range(PIECES)]

    def pair(self, k):
        return remote(self.place, self.theirs.at[k % self.n_buf], self.got.at[k], self.send.at[k], self.recv.at[k], "c")

    def add(self, k, lo, slot, low, n):
        add_rows(self.mine.at[k], self.stage.at[slot].at[pl.ds(low, n)], lo + low, n)

    def chip(self, k):
        self.pair(k).wait_recv()
        add_rows(self.mine.at[k], self.got.at[k], 0, 2 * self.h)

    def chip_x(self):
        self.chip(1)
        self.near_x.start()

    def chip_y(self):
        self.chip(2)
        self.near_y.start()

    def chip_d(self):
        self.chip(3)
        for p in range(PIECES):
            self.far_y[p].start()
            self.far_x[p].start()

    def turn(self):
        for p in range(PIECES):
            self.far_y[p].wait_recv()
            self.add(2, 0, 2, p * self.q, self.q)
            self.last_y[p].start()
            self.far_x[p].wait_recv()
            self.add(1, self.h, 3, p * self.q, self.q)
            self.last_x[p].start()

    def near(self):
        self.near_x.wait_recv()
        self.add(0, 0, 0, 0, self.h)
        self.near_y.wait_recv()
        self.add(0, self.h, 1, 0, self.h)

    def last(self, p):
        self.last_y[p].wait_recv()
        self.add(0, 0, 4, p * self.q, self.q)
        self.last_x[p].wait_recv()
        self.add(0, self.h, 5, p * self.q, self.q)

    def drain(self, last):
        if last:
            for k in range(4 - self.n_buf, 4):
                self.pair(k).wait_send()
        for c in [self.near_x, self.near_y] + self.far_x + self.far_y + self.last_x + self.last_y:
            c.wait_send()


def slot_ids(n_tok, cap):
    return lax.broadcasted_iota(jnp.int32, (n_tok, cap), 0).astype(F32)


def one_hot(tab, src, t, e, ids):
    return jnp.where(tab[src, t, 0, pl.ds(e, 1), :] == ids, 1.0, 0.0).astype(BF16)


def gated(tab, src, t, e, ids):
    return jnp.where(tab[src, t, 0, pl.ds(e, 1), :] == ids, tab[src, t, 1, pl.ds(e, 1), :], 0.0).astype(BF16)


def pick(weights, rows):
    return dot_ta(jnp.concatenate(weights, axis=1), rows).astype(BF16)


def experts_fwd(place, tab, t, k, z, w, os, mine, theirs, mid):
    n_exp, cap, n_tok = w[0].shape[0], tab.shape[4], z.shape[2]
    ids = slot_ids(n_tok, cap)
    src = [place.source(k, c) for c in range(2)]

    def step(i, _):
        mid(i)
        es = (2 * i, 2 * i + 1)
        x = [pick([one_hot(tab, src[c], t, e, ids) for e in es], z[k, c]) for c in range(2)]
        for j, e in enumerate(es):
            xe = jnp.concatenate([x[c][j * cap:(j + 1) * cap] for c in range(2)], axis=0)
            a = dot(xe, w[0][e])
            b = dot(xe, w[1][e])
            o = dot((a * jax.nn.sigmoid(a) * b).astype(BF16), w[2][e]).astype(BF16)
            rows = pl.ds(pl.multiple_of(e * cap, cap), cap)
            os[0, rows, :] = o[:cap]
            os[1, rows, :] = o[cap:]
        return 0
    lax.fori_loop(0, n_exp // 2, step, 0)
    mid(n_exp // 2)
    for c, p in ((1, theirs), (0, mine)):
        p[...] = dot(jnp.concatenate([gated(tab, src[c], t, e, ids) for e in range(n_exp)], axis=1), os[c])


def experts_bwd(place, tab, t, k, z, g, w, grads, os, mine, theirs, mid):
    n_exp, cap, n_tok = w[0].shape[0], tab.shape[4], z.shape[2]
    ids = slot_ids(n_tok, cap)
    src = [place.source(k, c) for c in range(2)]

    def step(i, _):
        mid(i)
        es = (2 * i, 2 * i + 1)
        x = [pick([one_hot(tab, src[c], t, e, ids) for e in es], z[k, c]) for c in range(2)]
        r = [pick([gated(tab, src[c], t, e, ids) for e in es], g[k, c]) for c in range(2)]
        for j, e in enumerate(es):
            xe = jnp.concatenate([x[c][j * cap:(j + 1) * cap] for c in range(2)], axis=0)
            re = jnp.concatenate([r[c][j * cap:(j + 1) * cap] for c in range(2)], axis=0)
            a = dot(xe, w[0][e])
            b = dot(xe, w[1][e])
            dm = dot_tb(re, w[2][e])
            sig = jax.nn.sigmoid(a)
            act = a * sig
            m = (act * b).astype(BF16)
            da = (dm * b * (sig * (1.0 + a * (1.0 - sig)))).astype(BF16)
            db = (dm * act).astype(BF16)
            o = (dot_tb(da, w[0][e]) + dot_tb(db, w[1][e])).astype(BF16)
            rows = pl.ds(pl.multiple_of(e * cap, cap), cap)
            os[0, rows, :] = o[:cap]
            os[1, rows, :] = o[cap:]
            grads[0][e] += dot_ta(xe, da)
            grads[1][e] += dot_ta(xe, db)
            grads[2][e] += dot_ta(m, re)
        return 0
    lax.fori_loop(0, n_exp // 2, step, 0)
    mid(n_exp // 2)
    for c, p in ((1, theirs), (0, mine)):
        p[...] = dot(jnp.concatenate([one_hot(tab, src[c], t, e, ids) for e in range(n_exp)], axis=1), os[c])


def add_hidden(h_ref, mixed):
    def step(i, _):
        rows = pl.ds(pl.multiple_of(i * ROWS, ROWS), ROWS)
        h_ref[rows, :] = (h_ref[rows, :].astype(F32) + mixed[rows, :]).astype(BF16)
        return 0
    lax.fori_loop(0, h_ref.shape[0] // ROWS, step, 0)


def spaces(tree):
    if isinstance(tree, dict):
        return SimpleNamespace(**{k: spaces(v) for k, v in tree.items()})
    return tuple(spaces(v) for v in tree) if isinstance(tree, tuple) else tree


class Local:
    def __init__(self, sems):
        self.sems, self.used = sems, 0

    def make(self, a, b):
        self.used += 1
        return pltpu.make_async_copy(a, b, self.sems.at[self.used - 1])

    def __call__(self, a, b):
        c = self.make(a, b)
        c.start()
        return c


def done(copies):
    for c in copies:
        c.wait()


FWD, SECOND, FIRST = range(3)


def moe_body(kinds, blocks, passes, trees, *refs):
    arg, out, own = (spaces(v) for v in jax.tree.unflatten(trees, refs))
    place = Place()
    fetch, put = Local(own.load), Local(own.store)
    start = kinds == (FWD,)
    peers = [place.source(j // 2, j % 2) for j in range(1, 8)] if start else list(place.near.values())
    ships = kinds[-1] == FIRST
    n_stage = lax.axis_size("pp")
    nxt, prv = lax.rem(place.pp + 1, n_stage), lax.rem(place.pp + n_stage - 1, n_stage)
    greet(place, peers)
    if ships:
        for stage in (nxt, prv):
            pl.semaphore_signal(pltpu.get_barrier_semaphore(), inc=1, device_id=(stage, place.source(0, 0)), device_id_type=MESH)

    def fetch_experts(block, make=fetch):
        return [make(a.at[0, block], v) for a, v in zip(arg.experts, own.experts)]

    def fetch_dense(block):
        return [fetch(a.at[0, block], v) for a, v in zip(arg.dense, own.dense)]

    streams = []
    for s, kind in enumerate(kinds):
        o = own.streams[s]
        st = SimpleNamespace(kind=kind, block=blocks[s], t=passes[s], arg=arg.streams[s], out=out.streams[s], z=o.z, h=o.h, x=o.x, g=o.g)
        st.rows = Rows(place, o.g if kind == FIRST else o.z, o.row_send, o.row_recv)
        st.sums = Sums(place, o.mine, own.theirs, o.got, o.stage, o.sum_send, o.sum_recv)
        st.x_in = o.z.at[0, 0] if o.x is None else o.x
        st.fed = st.arg.x is None
        streams.append(st)
    a, b = streams[0], streams[-1]
    two = len(streams) == 2
    tab = own.tab
    later, ends, post = [], [], []
    extra = None
    if start:
        extra = Rows(place, own.more, own.more_send, own.more_recv, True)
        more_in = fetch(arg.more, own.more.at[0, 0])
        later += [fetch(r, v) for r, v in zip(arg.routes, own.routes)]
        next_in = fetch(arg.next, own.next)
    x_in = [[fetch(st.arg.z, st.z.at[0, 0]), fetch(st.arg.h, st.h)] if st.fed else [fetch(st.arg.x, st.x_in)] for st in streams]
    have = b.block
    d_in = fetch_dense(have)
    e_in = fetch_experts(a.block)
    if not start:
        later.append(fetch(arg.tab, tab))
        if b.kind == SECOND:
            later.append(fetch(b.arg.g, b.g))
        else:
            later += [fetch(b.arg.g, b.g.at[0, 0]), fetch(b.arg.z, b.z), fetch(b.arg.h, b.h)] + x_in[1]

    def tables(t):
        routes = own.routes[2 * (t // 2):2 * (t // 2) + 2]
        slot_tables(*routes, own.mail, t - t % 2, t % 2)
        me = place.source(0, 0)
        later.append(fetch(own.mail.at[me, t], tab.at[me, t]))
        for j, to in enumerate(peers):
            c = pltpu.make_async_remote_copy(src_ref=own.mail.at[to, t], dst_ref=tab.at[me, t], send_sem=own.tab_send.at[t, j],
                                             recv_sem=own.tab_recv.at[t, j], device_id=(place.pp, to), device_id_type=MESH)
            c.start()
            post.append(c)

    if start:
        greeted(peers)
        more_in.wait()
        extra.start()
        done(later)
        later = []
        tables(2)
    for st in streams:
        if st.kind == FIRST:
            continue
        done(x_in[0 if st is a else 1])
        if not st.fed:
            done(d_in)
            d_in = []
            dense_fwd(st.x_in, *own.dense, st.h, st.z.at[0, 0])
        if st is a:
            if not start:
                greeted(peers + [nxt, prv] if ships else peers)
            st.rows.start()
    end_dense = d_in
    if start:
        for t in (3, 0, 1):
            tables(t)
    if b.kind != FWD:
        for gr in own.grads:
            def clear(e, _, gr=gr):
                gr[e] = jnp.zeros(gr.shape[1:], F32)
                return 0
            lax.fori_loop(0, gr.shape[0], clear, 0)
    done(later)
    done(e_in)
    swap = fetch_experts(b.block, fetch.make) if two else []

    def unit(st, k, mid):
        sums = st.sums
        nb = sums.n_buf

        @pl.when(k >= nb)
        def _():
            sums.pair(k - nb).wait_send()
        if st is not a:
            @pl.when(k < nb)
            def _():
                a.sums.pair(k + 4 - nb).wait_send()
        theirs = sums.theirs.at[k % nb]
        if st.kind == FWD:
            experts_fwd(place, tab, st.t, k, st.z, own.experts, own.os, sums.mine.at[k], theirs, mid)
        else:
            experts_bwd(place, tab, st.t, k, st.z, st.g, own.experts, own.grads, own.os, sums.mine.at[k], theirs, mid)
        sums.pair(k).start()

    def pass_xy(r):
        r.pass_x()
        r.pass_y()

    ra, rb, sa, sb = a.rows, b.rows, a.sums, b.sums
    if two:
        before = {(0, 1): [lambda: pass_xy(ra), rb.start], (1, 0): [lambda: pass_xy(rb)], (1, 2): [rb.pass_d]}
        during = {(0, 2): [ra.pass_d, sa.chip_x], (0, 3): [sa.chip_y], (1, 0): [sa.chip_d], (1, 1): [lambda: sa.chip(0)],
                  (1, 2): [sa.turn, sb.chip_x], (1, 3): [sb.chip_y]}
    else:
        def prepare():
            dense_fwd(own.next, *own.dense, own.next, own.next_z)
        before = {(0, 0): [c.wait_recv for c in post[:7]], (0, 1): [next_in.wait, prepare, lambda: pass_xy(ra), extra.rest]}
        during = {(0, 2): [ra.pass_d, sa.chip_x], (0, 3): [sa.chip_y]}
    n_step = own.experts[0].shape[0] // 2
    for s, st in enumerate(streams):
        at = 2 if st.kind == FWD else 1

        def loop(k, _, s=s, st=st, at=at):
            for kk in range(4):
                @pl.when(k == kk)
                def _(kk=kk):
                    for f in before.get((s, kk), []):
                        f()
                    st.rows.ready(kk)

            def mid(i):
                if s == 0 and two:
                    @pl.when((k == 3) & (i == n_step))
                    def _():
                        for c in swap:
                            c.start()
                for kk in range(4):
                    if (s, kk) in during:
                        @pl.when((k == kk) & (i == at))
                        def _(kk=kk):
                            for f in during[s, kk]:
                                f()
            unit(st, k, mid)
            return 0
        lax.fori_loop(0, 4, loop, 0)
        if s == 0:
            done(swap)
    if b.kind != FWD:
        ends += [put(gr, o) for gr, o in zip(own.grads, out.grads)]
    sb.chip_d()
    if start:
        ends += [put(a.z, out.z), put(own.next, out.next.h), put(own.next_z, out.next.z)]
        pass_xy(extra)
    sb.chip(0)
    done(end_dense)
    if two:
        dense_slope(b.x, own.dense[0], sb.got)
        sa.near()
        ship = None
        if ships:
            ship = pltpu.make_async_remote_copy(src_ref=a.h, dst_ref=a.out.y, send_sem=own.ship.at[0], recv_sem=own.ship.at[1],
                                                device_id=(nxt, place.source(0, 0)), device_id_type=MESH)
        finish(a, own.dense, put, ends, False, ship)
    elif a.out.h is not None:
        put(a.h, a.out.h).wait()
    sb.near()
    sb.turn()
    if start:
        extra.pass_d()
        for c in post[7:]:
            c.wait_recv()
        ends.append(put(tab, out.tab))
        for k in range(4):
            extra.ready(k)
        ends.append(put(own.more, out.more))
        extra.drain()
    finish(b, own.dense, put, ends, True)
    for c in post:
        c.wait_send()
    done(ends)


def finish(st, dense, put, ends, last, ship=None):
    sums = st.sums
    for p in range(PIECES):
        sums.last(p)
        if st.kind != FWD:
            dense_bwd(st.g.at[0, 0], sums.mine.at[0], st.h, st.x, sums.got, *dense, st.x, p, sums.q)
            for low in (0, sums.h):
                rows = pl.ds(low + p * sums.q, sums.q)
                ends.append(put(st.x.at[rows], st.out.y.at[rows]))
    st.rows.drain()
    if st.kind == FWD:
        add_hidden(st.h, sums.mine.at[0])
        if st.out.z is not None:
            dense_fwd(st.h, *dense, st.h, st.z.at[0, 0])
            ends += [put(st.h, st.out.h), put(st.z.at[0, 0], st.out.z)]
        elif ship is None:
            ends.append(put(st.h, st.out.y))
        else:
            ship.start()
            ends.append(ship)
    sums.drain(last)


def moe(kinds, blocks, passes, args, weights, cid, n_buf=2):
    n, d = args["streams"][-1]["x"].shape
    experts, dense = weights[:3], weights[3:]
    start = kinds == (FWD,)
    dma, vmem = pltpu.SemaphoreType.DMA, pltpu.VMEM
    shapes = [v.shape[2:] for v in experts]
    n_exp = shapes[0][0]
    tab = (8, 4, 2, 8, 128)
    every = (4, 2, n, d)
    slots = vmem(every, BF16)
    give = jax.ShapeDtypeStruct
    args = dict(args, experts=tuple(experts), dense=tuple(dense))
    row = give((n, d), BF16)
    if start:
        outs = dict(streams=(dict(y=row, h=row, z=None),), next=dict(h=row, z=row))
    elif kinds[-1] == SECOND:
        outs = dict(streams=(dict(y=None, h=row, z=row), dict(y=row, h=None, z=None)))
    else:
        outs = dict(streams=(dict(y=row, h=None, z=None), dict(y=row, h=None, z=None)))
    own = dict(experts=tuple(vmem(v, BF16) for v in shapes), dense=tuple(vmem(v.shape[2:], BF16) for v in dense), os=vmem((2, n_exp * 128, d), BF16),
               theirs=vmem((n_buf, n, d), F32), load=dma((24,)), store=dma((24,)), ship=dma((2,)), tab=vmem(tab, F32))
    if start:
        outs.update(tab=give(tab, F32), z=give(every, BF16), more=give(every, BF16))
        own.update(mail=vmem(tab, F32), next=vmem((n, d), BF16), next_z=vmem((n, d), BF16), tab_send=dma((4, 7)), tab_recv=dma((4, 7)), more=slots, more_send=dma((N_AG,)), more_recv=dma((N_AG,)),
                   routes=tuple(vmem(v.shape, v.dtype) for v in args["routes"]))
    else:
        outs.update(grads=tuple(give(v, F32) for v in shapes))
        own.update(grads=tuple(vmem(v, F32) for v in shapes))
    own.update(streams=tuple(dict(
        z=slots, h=vmem((n, d), BF16), x=vmem((n, d), BF16) if kind != FWD else None, g=slots if kind != FWD else None, row_send=dma((N_AG,)), row_recv=dma((N_AG,)),
        mine=vmem((4, n, d), F32), got=vmem((4, n, d), F32), stage=vmem((6, n // 2, d), F32), sum_send=dma((N_RS,)), sum_recv=dma((N_RS,))) for kind in kinds))
    flat_in, _ = jax.tree.flatten(args)
    flat_out, out_tree = jax.tree.flatten(outs)
    flat_own, _ = jax.tree.flatten(own)
    _, trees = jax.tree.flatten((args, outs, own))
    res = pl.pallas_call(
        functools.partial(moe_body, kinds, blocks, passes, trees), out_shape=flat_out, in_specs=[ANY] * len(flat_in), out_specs=[ANY] * len(flat_out),
        scratch_shapes=flat_own, compiler_params=pltpu.CompilerParams(vmem_limit_bytes=67043328, collective_id=cid, has_side_effects=True),
        cost_estimate=cost(3e10, 5e7), name=f"moe_{cid}")(*flat_in)
    return spaces(jax.tree.unflatten(out_tree, res))


def solution(mesh):
    stages = mesh.shape['pp']
    to_prev = [(sender, (sender - 1) % stages) for sender in range(stages)]

    def local_step(x_fwd, x_bwd, grad_in, dense_in, dense_out, exp_gate, exp_up, exp_down, route_fwd, gate_fwd, route_bwd, gate_bwd):
        weights = (exp_gate, exp_up, exp_down, dense_in, dense_out)
        routes = tuple(jnp.swapaxes(v[0], 1, 2) for v in (route_fwd, gate_fwd, route_bwd, gate_bwd))
        one = moe((FWD,), (0,), (2,), dict(routes=routes, more=grad_in[0], next=x_fwd[0], streams=(dict(x=x_bwd[0]),)), weights, 0)
        mid = one.streams[0]
        two = moe((FWD, SECOND), (0, 1), (0, 3), dict(tab=one.tab, streams=(dict(x=None, z=one.next.z, h=one.next.h), dict(x=mid.y, g=one.more))), weights, 1)
        back = dict(x=x_bwd[0], h=mid.h, z=one.z, g=two.streams[1].y)
        three = moe((FWD, FIRST), (1, 0), (1, 2), dict(tab=one.tab, streams=(dict(x=None, z=two.streams[0].z, h=two.streams[0].h), back)), weights, 2)
        dx_prev = lax.ppermute(three.streams[1].y, 'pp', to_prev)
        return (three.streams[0].y[None], dx_prev[None]) + tuple(jnp.stack([p, q])[None] for p, q in zip(three.grads, two.grads))

    tok_spec = P('pp', 'ep', None)
    dense_spec = P('pp', None, None, None)
    exp_spec = P('pp', None, 'ep', None, None)
    route_spec = P('pp', None, 'ep', None)
    return jax.shard_map(local_step, mesh=mesh, in_specs=(tok_spec, tok_spec, tok_spec, dense_spec, dense_spec, exp_spec, exp_spec, exp_spec, route_spec, route_spec, route_spec, route_spec), out_specs=(tok_spec, tok_spec, exp_spec, exp_spec, exp_spec), check_vma=False)
```

```python
import functools
from types import SimpleNamespace

import jax
import jax.numpy as jnp
from jax import lax
from jax.experimental import pallas as pl
from jax.experimental.pallas import tpu as pltpu
from jax.sharding import PartitionSpec as P

NORM_EPS = 1e-6
F32 = jnp.float32
BF16 = jnp.bfloat16
ANY = pl.BlockSpec(memory_space=pl.ANY)


def dot(a, b, over=((1,), (0,))):
    return lax.dot_general(a, b, (over, ((), ())), preferred_element_type=F32)


def dot_ta(a, b):
    return dot(a, b, ((0,), (0,)))


def dot_tb(a, b):
    return dot(a, b, ((1,), (1,)))


def rms_norm(v):
    return v * lax.rsqrt(jnp.mean(v * v, axis=-1, keepdims=True) + NORM_EPS)


def rms_back(v, g):
    inv = lax.rsqrt(jnp.mean(v * v, axis=-1, keepdims=True) + NORM_EPS)
    proj = jnp.mean(g * v, axis=-1, keepdims=True)
    return inv * g - v * (inv * inv * inv) * proj


def cost(flops, nbytes):
    return pl.CostEstimate(flops=int(flops), bytes_accessed=int(nbytes), transcendentals=0)


ROWS = 256


def dense_fwd(x_ref, w1, w2, h_ref, z_ref):
    def step(i, _):
        rows = pl.ds(pl.multiple_of(i * ROWS, ROWS), ROWS)
        x = x_ref[rows, :].astype(F32)
        pre = dot(rms_norm(x).astype(BF16), w1[...])
        mid = (pre * jax.nn.sigmoid(pre)).astype(BF16)
        h = (x + dot(mid, w2[...])).astype(BF16)
        h_ref[rows, :] = h
        z_ref[rows, :] = rms_norm(h.astype(F32)).astype(BF16)
        return 0
    lax.fori_loop(0, x_ref.shape[0] // ROWS, step, 0)


def dense_slope(x_ref, w1, slope):
    half = slope.shape[2]

    def step(i, _):
        rows = pl.ds(pl.multiple_of(i * ROWS, ROWS), ROWS)
        pre = dot(rms_norm(x_ref[rows, :].astype(F32)).astype(BF16), w1[...])
        sig = jax.nn.sigmoid(pre)
        val = sig * (1.0 + pre * (1.0 - sig))
        slope[0, rows, :] = val[:, :half]
        slope[1, rows, :] = val[:, half:]
        return 0
    lax.fori_loop(0, x_ref.shape[0] // ROWS, step, 0)


def dense_bwd(g_ref, dz_ref, h_ref, x_ref, slope, w1, w2, o_ref, piece, size):
    def step(i, _):
        rows = pl.ds(pl.multiple_of(i * (x_ref.shape[0] // 2) + piece * size, size), size)
        x = x_ref[rows, :].astype(F32)
        dh = g_ref[rows, :].astype(F32) + rms_back(h_ref[rows, :].astype(F32), dz_ref[rows, :])
        turned = jnp.concatenate([slope[0, rows, :], slope[1, rows, :]], axis=1)
        dp = (dot_tb(dh.astype(BF16), w2[...]) * turned).astype(BF16)
        o_ref[rows, :] = (dh + rms_back(x, dot_tb(dp, w1[...]))).astype(BF16)
        return 0
    lax.fori_loop(0, 2, step, 0)


def slot_tables(route_ref, gate_ref, o_ref, base, t):
    _, top_k, n_tok = route_ref.shape
    groups = o_ref.shape[0]
    n_exp = groups * o_ref.shape[3]
    row = lax.broadcasted_iota(jnp.int32, (2 * n_exp, n_tok), 0)
    first = row < n_exp
    row_exp = jnp.where(first, row, row - n_exp)
    ids = lax.broadcasted_iota(jnp.int32, (2 * n_exp, n_tok), 1) + 1
    value = jnp.where(first, ids >> 4, ids & 15).astype(F32)
    slot = lax.broadcasted_iota(jnp.int32, (128, n_tok), 0)

    acc = jnp.zeros((3 * n_exp, 128), F32)
    for k in range(top_k):
        r = route_ref[t, k:k + 1, :]
        hit = (r >> 7) == row_exp
        left = jnp.concatenate([jnp.where(hit, value, 0.0), jnp.where(hit[:n_exp], gate_ref[t, k:k + 1, :].astype(F32), 0.0)], axis=0)
        right = jnp.where((r & 127) == slot, 1.0, 0.0).astype(BF16)
        acc += dot_tb(left.astype(BF16), right)
    tok = acc[:n_exp] * 16.0 + acc[n_exp:2 * n_exp] - 1.0
    gat = acc[2 * n_exp:]
    for g in range(groups):
        o_ref[g, base + t, 0] = tok[g * 8:(g + 1) * 8]
        o_ref[g, base + t, 1] = gat[g * 8:(g + 1) * 8]


MESH = pl.DeviceIdType.MESH
N_AG, N_RS, PIECES = 10, 22, 4


class Place:
    def __init__(self):
        me = lax.axis_index("ep")
        self.core, self.x, self.y = me % 2, (me // 2) % 2, me // 4
        self.pp = lax.axis_index("pp")
        self.near = {"c": me + 1 - 2 * self.core, "x": me + 2 - 4 * self.x, "y": me + 4 - 8 * self.y}

    def source(self, k, c):
        x, y = (self.x + k % 2) % 2, (self.y + k // 2) % 2
        core = self.core if c == 0 else 1 - self.core
        return y * 4 + x * 2 + core


def remote(place, src, dst, send, recv, to):
    return pltpu.make_async_remote_copy(src_ref=src, dst_ref=dst, send_sem=send, recv_sem=recv, device_id=(place.pp, place.near[to]), device_id_type=MESH)


def greet(place, peers):
    for peer in peers:
        pl.semaphore_signal(pltpu.get_barrier_semaphore(), inc=1, device_id=(place.pp, peer), device_id_type=MESH)


def greeted(peers):
    pl.semaphore_wait(pltpu.get_barrier_semaphore(), len(peers))


class Rows:
    def __init__(self, place, slots, send, recv, split=False):
        h = slots.shape[2] // 2
        self.split = split
        plan = ((0, 0, 1, 0, "x", None), (0, 0, 2, 0, "y", None), (0, 0, 0, 1, "c", None), (1, 0, 3, 0, "y", (0, h)), (1, 0, 1, 1, "c", None),
                (2, 0, 3, 0, "x", (h, h)), (2, 0, 2, 1, "c", None), (3, 0, 3, 1, "c", None))
        if split:
            q = h // 2
            plan = ((0, 0, 1, 0, "x", (0, q)), (0, 0, 2, 0, "y", (0, q))) + plan[2:] + ((0, 0, 1, 0, "x", (q, 3 * q)), (0, 0, 2, 0, "y", (q, 3 * q)))
        self.copies = []
        for i, (ks, cs, kd, cd, to, part) in enumerate(plan):
            s, d = slots.at[ks, cs], slots.at[kd, cd]
            if part is not None:
                s, d = s.at[pl.ds(*part)], d.at[pl.ds(*part)]
            self.copies.append(remote(place, s, d, send.at[i], recv.at[i], to))

    def start(self):
        for i in (0, 1, 2):
            self.copies[i].start()

    def rest(self):
        self.copies[8].start()
        self.copies[9].start()

    def pass_x(self):
        self.copies[0].wait_recv()
        if self.split:
            self.copies[8].wait_recv()
        self.copies[3].start()
        self.copies[4].start()

    def pass_y(self):
        self.copies[1].wait_recv()
        if self.split:
            self.copies[9].wait_recv()
        self.copies[5].start()
        self.copies[6].start()

    def pass_d(self):
        self.copies[3].wait_recv()
        self.copies[5].wait_recv()
        self.copies[7].start()

    def ready(self, k):
        self.copies[(2, 4, 6, 7)[k]].wait_recv()

    def drain(self):
        for c in self.copies:
            c.wait_send()


def add_rows(dst, b, lo, n):
    def step(i, _):
        at = pl.multiple_of(i * 64, 64)
        rows = pl.ds(lo + at, 64)
        dst[rows, :] = dst[rows, :] + b[pl.ds(at, 64), :]
        return 0
    lax.fori_loop(0, n // 64, step, 0)


class Sums:
    def __init__(self, place, mine, theirs, got, stage, send, recv):
        h = mine.shape[1] // 2
        self.h, self.q, self.mine, self.got, self.stage, self.recv, self.send = h, h // PIECES, mine, got, stage, recv, send
        self.theirs, self.n_buf, self.place = theirs, theirs.shape[0], place

        def move(sem, slot, k, at, low, n, to):
            return remote(place, mine.at[k].at[pl.ds(at + low, n)], stage.at[slot].at[pl.ds(low, n)], send.at[sem], recv.at[sem], to)
        self.near_x, self.near_y = move(4, 0, 1, 0, 0, h, "x"), move(5, 1, 2, h, 0, h, "y")
        q = self.q
        table = ((3, 0, "x"), (3, h, "y"), (2, 0, "y"), (1, h, "x"))
        late = [[move(6 + j * PIECES + p, 2 + j, k, at, p * q, q, to) for p in range(PIECES)] for j, (k, at, to) in enumerate(table)]
        self.far_y, self.far_x, self.last_y, self.last_x = late

    def pair(self, k):
        return remote(self.place, self.theirs.at[k % self.n_buf], self.got.at[k], self.send.at[k], self.recv.at[k], "c")

    def add(self, k, lo, slot, low, n):
        add_rows(self.mine.at[k], self.stage.at[slot].at[pl.ds(low, n)], lo + low, n)

    def chip(self, k):
        self.pair(k).wait_recv()
        add_rows(self.mine.at[k], self.got.at[k], 0, 2 * self.h)

    def chip_x(self):
        self.chip(1)
        self.near_x.start()

    def chip_y(self):
        self.chip(2)
        self.near_y.start()

    def chip_d(self):
        self.chip(3)
        for p in range(PIECES):
            self.far_y[p].start()
            self.far_x[p].start()

    def turn(self):
        for p in range(PIECES):
            self.far_y[p].wait_recv()
            self.add(2, 0, 2, p * self.q, self.q)
            self.last_y[p].start()
            self.far_x[p].wait_recv()
            self.add(1, self.h, 3, p * self.q, self.q)
            self.last_x[p].start()

    def near(self):
        self.near_x.wait_recv()
        self.add(0, 0, 0, 0, self.h)
        self.near_y.wait_recv()
        self.add(0, self.h, 1, 0, self.h)

    def last(self, p):
        self.last_y[p].wait_recv()
        self.add(0, 0, 4, p * self.q, self.q)
        self.last_x[p].wait_recv()
        self.add(0, self.h, 5, p * self.q, self.q)

    def drain(self, last):
        if last:
            for k in range(4 - self.n_buf, 4):
                self.pair(k).wait_send()
        for c in [self.near_x, self.near_y] + self.far_x + self.far_y + self.last_x + self.last_y:
            c.wait_send()


def slot_ids(n_tok, cap):
    return lax.broadcasted_iota(jnp.int32, (n_tok, cap), 0).astype(F32)


def one_hot(tab, src, t, e, ids):
    return jnp.where(tab[src, t, 0, pl.ds(e, 1), :] == ids, 1.0, 0.0).astype(BF16)


def gated(tab, src, t, e, ids):
    return jnp.where(tab[src, t, 0, pl.ds(e, 1), :] == ids, tab[src, t, 1, pl.ds(e, 1), :], 0.0).astype(BF16)


def pick(weights, rows):
    return dot_ta(jnp.concatenate(weights, axis=1), rows).astype(BF16)


def experts_fwd(place, tab, t, k, z, w, os, mine, theirs, mid):
    n_exp, cap, n_tok = w[0].shape[0], tab.shape[4], z.shape[2]
    ids = slot_ids(n_tok, cap)
    src = [place.source(k, c) for c in range(2)]

    def step(i, _):
        mid(i)
        es = (2 * i, 2 * i + 1)
        x = [pick([one_hot(tab, src[c], t, e, ids) for e in es], z[k, c]) for c in range(2)]
        for j, e in enumerate(es):
            xe = jnp.concatenate([x[c][j * cap:(j + 1) * cap] for c in range(2)], axis=0)
            a = dot(xe, w[0][e])
            b = dot(xe, w[1][e])
            o = dot((a * jax.nn.sigmoid(a) * b).astype(BF16), w[2][e]).astype(BF16)
            rows = pl.ds(pl.multiple_of(e * cap, cap), cap)
            os[0, rows, :] = o[:cap]
            os[1, rows, :] = o[cap:]
        return 0
    lax.fori_loop(0, n_exp // 2, step, 0)
    mid(n_exp // 2)
    for c, p in ((1, theirs), (0, mine)):
        p[...] = dot(jnp.concatenate([gated(tab, src[c], t, e, ids) for e in range(n_exp)], axis=1), os[c])


def experts_bwd(place, tab, t, k, z, g, w, grads, os, mine, theirs, mid):
    n_exp, cap, n_tok = w[0].shape[0], tab.shape[4], z.shape[2]
    ids = slot_ids(n_tok, cap)
    src = [place.source(k, c) for c in range(2)]

    def step(i, _):
        mid(i)
        es = (2 * i, 2 * i + 1)
        x = [pick([one_hot(tab, src[c], t, e, ids) for e in es], z[k, c]) for c in range(2)]
        r = [pick([gated(tab, src[c], t, e, ids) for e in es], g[k, c]) for c in range(2)]
        for j, e in enumerate(es):
            xe = jnp.concatenate([x[c][j * cap:(j + 1) * cap] for c in range(2)], axis=0)
            re = jnp.concatenate([r[c][j * cap:(j + 1) * cap] for c in range(2)], axis=0)
            a = dot(xe, w[0][e])
            b = dot(xe, w[1][e])
            dm = dot_tb(re, w[2][e])
            sig = jax.nn.sigmoid(a)
            act = a * sig
            m = (act * b).astype(BF16)
            da = (dm * b * (sig * (1.0 + a * (1.0 - sig)))).astype(BF16)
            db = (dm * act).astype(BF16)
            o = (dot_tb(da, w[0][e]) + dot_tb(db, w[1][e])).astype(BF16)
            rows = pl.ds(pl.multiple_of(e * cap, cap), cap)
            os[0, rows, :] = o[:cap]
            os[1, rows, :] = o[cap:]
            grads[0][e] += dot_ta(xe, da)
            grads[1][e] += dot_ta(xe, db)
            grads[2][e] += dot_ta(m, re)
        return 0
    lax.fori_loop(0, n_exp // 2, step, 0)
    mid(n_exp // 2)
    for c, p in ((1, theirs), (0, mine)):
        p[...] = dot(jnp.concatenate([one_hot(tab, src[c], t, e, ids) for e in range(n_exp)], axis=1), os[c])


def add_hidden(h_ref, mixed):
    def step(i, _):
        rows = pl.ds(pl.multiple_of(i * ROWS, ROWS), ROWS)
        h_ref[rows, :] = (h_ref[rows, :].astype(F32) + mixed[rows, :]).astype(BF16)
        return 0
    lax.fori_loop(0, h_ref.shape[0] // ROWS, step, 0)


def spaces(tree):
    if isinstance(tree, dict):
        return SimpleNamespace(**{k: spaces(v) for k, v in tree.items()})
    return tuple(spaces(v) for v in tree) if isinstance(tree, tuple) else tree


class Local:
    def __init__(self, sems):
        self.sems, self.used = sems, 0

    def make(self, a, b):
        self.used += 1
        return pltpu.make_async_copy(a, b, self.sems.at[self.used - 1])

    def __call__(self, a, b):
        c = self.make(a, b)
        c.start()
        return c


def done(copies):
    for c in copies:
        c.wait()


FWD, SECOND, FIRST = range(3)


def moe_body(kinds, blocks, passes, trees, *refs):
    arg, out, own = (spaces(v) for v in jax.tree.unflatten(trees, refs))
    place = Place()
    fetch, put = Local(own.load), Local(own.store)
    start = kinds == (FWD,)
    peers = [place.source(j // 2, j % 2) for j in range(1, 8)] if start else list(place.near.values())
    ships = kinds[-1] == FIRST
    n_stage = lax.axis_size("pp")
    nxt, prv = lax.rem(place.pp + 1, n_stage), lax.rem(place.pp + n_stage - 1, n_stage)
    greet(place, peers)
    if ships:
        for stage in (nxt, prv):
            pl.semaphore_signal(pltpu.get_barrier_semaphore(), inc=1, device_id=(stage, place.source(0, 0)), device_id_type=MESH)

    def fetch_experts(block, make=fetch):
        return [make(a.at[0, block], v) for a, v in zip(arg.experts, own.experts)]

    def fetch_dense(block):
        return [fetch(a.at[0, block], v) for a, v in zip(arg.dense, own.dense)]

    streams = []
    for s, kind in enumerate(kinds):
        o = own.streams[s]
        st = SimpleNamespace(kind=kind, block=blocks[s], t=passes[s], arg=arg.streams[s], out=out.streams[s], z=o.z, h=o.h, x=o.x, g=o.g)
        st.rows = Rows(place, o.g if kind == FIRST else o.z, o.row_send, o.row_recv)
        st.sums = Sums(place, o.mine, own.theirs, o.got, o.stage, o.sum_send, o.sum_recv)
        st.x_in = o.z.at[0, 0] if o.x is None else o.x
        st.fed = not hasattr(st.arg, "x")
        streams.append(st)
    a, b = streams[0], streams[-1]
    two = len(streams) == 2
    tab = own.tab
    later, ends, post = [], [], []
    extra = None
    if start:
        extra = Rows(place, own.more, own.more_send, own.more_recv, True)
        more_in = fetch(arg.more, own.more.at[0, 0])
        later += [fetch(r, v) for r, v in zip(arg.routes, own.routes)]
        next_in = fetch(arg.next, own.next)
    x_in = [[fetch(st.arg.z, st.z.at[0, 0]), fetch(st.arg.h, st.h)] if st.fed else [fetch(st.arg.x, st.x_in)] for st in streams]
    have = b.block
    d_in = fetch_dense(have)
    e_in = fetch_experts(a.block)
    if not start:
        later.append(fetch(arg.tab, tab))
        if b.kind == SECOND:
            later.append(fetch(b.arg.g, b.g))
        else:
            later += [fetch(b.arg.g, b.g.at[0, 0]), fetch(b.arg.z, b.z), fetch(b.arg.h, b.h)] + x_in[1]

    def tables(t):
        routes = own.routes[2 * (t // 2):2 * (t // 2) + 2]
        slot_tables(*routes, own.mail, t - t % 2, t % 2)
        me = place.source(0, 0)
        later.append(fetch(own.mail.at[me, t], tab.at[me, t]))
        for j, to in enumerate(peers):
            c = pltpu.make_async_remote_copy(src_ref=own.mail.at[to, t], dst_ref=tab.at[me, t], send_sem=own.tab_send.at[t, j],
                                             recv_sem=own.tab_recv.at[t, j], device_id=(place.pp, to), device_id_type=MESH)
            c.start()
            post.append(c)

    if start:
        greeted(peers)
        more_in.wait()
        extra.start()
        done(later)
        later = []
        tables(2)
    for st in streams:
        if st.kind == FIRST:
            continue
        done(x_in[0 if st is a else 1])
        if not st.fed:
            done(d_in)
            d_in = []
            dense_fwd(st.x_in, *own.dense, st.h, st.z.at[0, 0])
        if st is a:
            if not start:
                greeted(peers + [nxt, prv] if ships else peers)
            st.rows.start()
    end_dense = d_in
    if start:
        for t in (3, 0, 1):
            tables(t)
    if b.kind != FWD:
        for gr in own.grads:
            def clear(e, _, gr=gr):
                gr[e] = jnp.zeros(gr.shape[1:], F32)
                return 0
            lax.fori_loop(0, gr.shape[0], clear, 0)
    done(later)
    done(e_in)
    swap = fetch_experts(b.block, fetch.make) if two else []

    def unit(st, k, mid):
        sums = st.sums
        nb = sums.n_buf

        @pl.when(k >= nb)
        def _():
            sums.pair(k - nb).wait_send()
        if st is not a:
            @pl.when(k < nb)
            def _():
                a.sums.pair(k + 4 - nb).wait_send()
        theirs = sums.theirs.at[k % nb]
        if st.kind == FWD:
            experts_fwd(place, tab, st.t, k, st.z, own.experts, own.os, sums.mine.at[k], theirs, mid)
        else:
            experts_bwd(place, tab, st.t, k, st.z, st.g, own.experts, own.grads, own.os, sums.mine.at[k], theirs, mid)
        sums.pair(k).start()

    def pass_xy(r):
        r.pass_x()
        r.pass_y()

    ra, rb, sa, sb = a.rows, b.rows, a.sums, b.sums
    if two:
        before = {(0, 1): [lambda: pass_xy(ra), rb.start], (1, 0): [lambda: pass_xy(rb)], (1, 2): [rb.pass_d]}
        during = {(0, 2): [ra.pass_d, sa.chip_x], (0, 3): [sa.chip_y], (1, 0): [sa.chip_d], (1, 1): [lambda: sa.chip(0)],
                  (1, 2): [sa.turn, sb.chip_x], (1, 3): [sb.chip_y]}
    else:
        def prepare():
            dense_fwd(own.next, *own.dense, own.next, own.next_z)
        before = {(0, 0): [c.wait_recv for c in post[:7]], (0, 1): [next_in.wait, prepare, lambda: pass_xy(ra), extra.rest]}
        during = {(0, 2): [ra.pass_d, sa.chip_x], (0, 3): [sa.chip_y]}
    n_step = own.experts[0].shape[0] // 2
    for s, st in enumerate(streams):
        at = 2 if st.kind == FWD else 1

        def loop(k, _, s=s, st=st, at=at):
            for kk in range(4):
                @pl.when(k == kk)
                def _(kk=kk):
                    for f in before.get((s, kk), []):
                        f()
                    st.rows.ready(kk)

            def mid(i):
                if s == 0 and two:
                    @pl.when((k == 3) & (i == n_step))
                    def _():
                        for c in swap:
                            c.start()
                for kk in range(4):
                    if (s, kk) in during:
                        @pl.when((k == kk) & (i == at))
                        def _(kk=kk):
                            for f in during[s, kk]:
                                f()
            unit(st, k, mid)
            return 0
        lax.fori_loop(0, 4, loop, 0)
        if s == 0:
            done(swap)
    if b.kind != FWD:
        ends += [put(gr, o) for gr, o in zip(own.grads, out.grads)]
    sb.chip_d()
    if start:
        ends += [put(a.z, out.z), put(own.next, out.next.h), put(own.next_z, out.next.z)]
        pass_xy(extra)
    sb.chip(0)
    done(end_dense)
    if two:
        dense_slope(b.x, own.dense[0], sb.got)
        sa.near()
        ship = None
        if ships:
            ship = pltpu.make_async_remote_copy(src_ref=a.h, dst_ref=a.out.y, send_sem=own.ship.at[0], recv_sem=own.ship.at[1],
                                                device_id=(nxt, place.source(0, 0)), device_id_type=MESH)
        finish(a, own.dense, put, ends, False, ship)
    else:
        put(a.h, a.out.h).wait()
    sb.near()
    sb.turn()
    if start:
        extra.pass_d()
        for c in post[7:]:
            c.wait_recv()
        ends.append(put(tab, out.tab))
        for k in range(4):
            extra.ready(k)
        ends.append(put(own.more, out.more))
        extra.drain()
    finish(b, own.dense, put, ends, True)
    for c in post:
        c.wait_send()
    done(ends)


def finish(st, dense, put, ends, last, ship=None):
    sums = st.sums
    for p in range(PIECES):
        sums.last(p)
        if st.kind != FWD:
            dense_bwd(st.g.at[0, 0], sums.mine.at[0], st.h, st.x, sums.got, *dense, st.x, p, sums.q)
            for low in (0, sums.h):
                rows = pl.ds(low + p * sums.q, sums.q)
                ends.append(put(st.x.at[rows], st.out.y.at[rows]))
    st.rows.drain()
    if st.kind == FWD:
        add_hidden(st.h, sums.mine.at[0])
        if hasattr(st.out, "z"):
            dense_fwd(st.h, *dense, st.h, st.z.at[0, 0])
            ends += [put(st.h, st.out.h), put(st.z.at[0, 0], st.out.z)]
        elif ship is None:
            ends.append(put(st.h, st.out.y))
        else:
            ship.start()
            ends.append(ship)
    sums.drain(last)


def moe(kinds, blocks, passes, args, weights, cid, n_buf=2):
    n, d = args["streams"][-1]["x"].shape
    experts, dense = weights[:3], weights[3:]
    start = kinds == (FWD,)
    dma, vmem = pltpu.SemaphoreType.DMA, pltpu.VMEM
    shapes = [v.shape[2:] for v in experts]
    n_exp = shapes[0][0]
    tab = (8, 4, 2, 8, 128)
    every = (4, 2, n, d)
    slots = vmem(every, BF16)
    give = jax.ShapeDtypeStruct
    args = dict(args, experts=tuple(experts), dense=tuple(dense))
    row = give((n, d), BF16)
    if start:
        outs = dict(streams=(dict(y=row, h=row),), next=dict(h=row, z=row))
    elif kinds[-1] == SECOND:
        outs = dict(streams=(dict(h=row, z=row), dict(y=row)))
    else:
        outs = dict(streams=(dict(y=row), dict(y=row)))
    own = dict(experts=tuple(vmem(v, BF16) for v in shapes), dense=tuple(vmem(v.shape[2:], BF16) for v in dense), os=vmem((2, n_exp * 128, d), BF16),
               theirs=vmem((n_buf, n, d), F32), load=dma((24,)), store=dma((24,)), ship=dma((2,)), tab=vmem(tab, F32))
    if start:
        outs.update(tab=give(tab, F32), z=give(every, BF16), more=give(every, BF16))
        own.update(mail=vmem(tab, F32), next=vmem((n, d), BF16), next_z=vmem((n, d), BF16), tab_send=dma((4, 7)), tab_recv=dma((4, 7)), more=slots, more_send=dma((N_AG,)), more_recv=dma((N_AG,)),
                   routes=tuple(vmem(v.shape, v.dtype) for v in args["routes"]))
    else:
        outs.update(grads=tuple(give(v, F32) for v in shapes))
        own.update(grads=tuple(vmem(v, F32) for v in shapes))
    own.update(streams=tuple(dict(
        z=slots, h=vmem((n, d), BF16), x=vmem((n, d), BF16) if kind != FWD else None, g=slots if kind != FWD else None, row_send=dma((N_AG,)), row_recv=dma((N_AG,)),
        mine=vmem((4, n, d), F32), got=vmem((4, n, d), F32), stage=vmem((6, n // 2, d), F32), sum_send=dma((N_RS,)), sum_recv=dma((N_RS,))) for kind in kinds))
    flat_in, _ = jax.tree.flatten(args)
    flat_out, out_tree = jax.tree.flatten(outs)
    flat_own, _ = jax.tree.flatten(own)
    _, trees = jax.tree.flatten((args, outs, own))
    res = pl.pallas_call(
        functools.partial(moe_body, kinds, blocks, passes, trees), out_shape=flat_out, in_specs=[ANY] * len(flat_in), out_specs=[ANY] * len(flat_out),
        scratch_shapes=flat_own, compiler_params=pltpu.CompilerParams(vmem_limit_bytes=67043328, collective_id=cid, has_side_effects=True),
        cost_estimate=cost(3e10, 5e7), name=f"moe_{cid}")(*flat_in)
    return spaces(jax.tree.unflatten(out_tree, res))


def solution(mesh):
    stages = mesh.shape['pp']
    to_prev = [(sender, (sender - 1) % stages) for sender in range(stages)]

    def local_step(x_fwd, x_bwd, grad_in, dense_in, dense_out, exp_gate, exp_up, exp_down, route_fwd, gate_fwd, route_bwd, gate_bwd):
        weights = (exp_gate, exp_up, exp_down, dense_in, dense_out)
        routes = tuple(jnp.swapaxes(v[0], 1, 2) for v in (route_fwd, gate_fwd, route_bwd, gate_bwd))
        one = moe((FWD,), (0,), (2,), dict(routes=routes, more=grad_in[0], next=x_fwd[0], streams=(dict(x=x_bwd[0]),)), weights, 0)
        mid = one.streams[0]
        two = moe((FWD, SECOND), (0, 1), (0, 3), dict(tab=one.tab, streams=(dict(z=one.next.z, h=one.next.h), dict(x=mid.y, g=one.more))), weights, 1)
        back = dict(x=x_bwd[0], h=mid.h, z=one.z, g=two.streams[1].y)
        three = moe((FWD, FIRST), (1, 0), (1, 2), dict(tab=one.tab, streams=(dict(z=two.streams[0].z, h=two.streams[0].h), back)), weights, 2)
        dx_prev = lax.ppermute(three.streams[1].y, 'pp', to_prev)
        return (three.streams[0].y[None], dx_prev[None]) + tuple(jnp.stack([p, q])[None] for p, q in zip(three.grads, two.grads))

    tok_spec = P('pp', 'ep', None)
    dense_spec = P('pp', None, None, None)
    exp_spec = P('pp', None, 'ep', None, None)
    route_spec = P('pp', None, 'ep', None)
    return jax.shard_map(local_step, mesh=mesh, in_specs=(tok_spec, tok_spec, tok_spec, dense_spec, dense_spec, exp_spec, exp_spec, exp_spec, route_spec, route_spec, route_spec, route_spec), out_specs=(tok_spec, tok_spec, exp_spec, exp_spec, exp_spec), check_vma=False)
```
